512 devices in a mesh: shot: 2 (over y), gx: 16 (over z), gy: 8 (over x), gz: 2 (over core).
Axes of the slice: x: 8, y: 2, z: 16, core: 2. Of those that a mesh axis runs over, the one named last changes fastest.
The devices are a block of a 8x16x16 slice.
Arguments:
- source_prev: float32 [384, 32, 1024], P(('shot', 'gx'), 'gy', 'gz'), parts along dimension 0, may hold values from -6 to 6
- source_now: float32 [384, 32, 1024], P(('shot', 'gx'), 'gy', 'gz'), parts along dimension 0, may hold values from -6 to 6
- receiver_prev: float32 [384, 32, 1024], P(('shot', 'gx'), 'gy', 'gz'), parts along dimension 0, may hold values from -6 to 6
- receiver_now: float32 [384, 32, 1024], P(('shot', 'gx'), 'gy', 'gz'), parts along dimension 0, may hold values from -6 to 6
- courant: float32 [192, 32, 1024], P('gx', 'gy', 'gz'), may hold values from 0.04 to 0.16
- absorbing: int32 [192, 32, 1024], P('gx', 'gy', 'gz'), may hold values from 0 to 8, as said below
- source_cell: int32 [6], P('shot'), parts along dimension 0, may hold values from 0 to 1023, as said below
- wavelet: float32 [8], P('shot'), parts along dimension 0, may hold values from -4 to 4
- receiver_cells: int32 [4096, 2], P('shot'), parts along dimension 0, may hold values from 0 to 191, as said below
- traces: float32 [4, 4096], P(None, 'shot'), parts along dimension 1, may hold values from -6 to 6
Outputs:
- source_field: float32 [384, 32, 1024], P(('shot', 'gx'), 'gy', 'gz'), parts along dimension 0
- receiver_field: float32 [384, 32, 1024], P(('shot', 'gx'), 'gy', 'gz'), parts along dimension 0
- filtered_image: bfloat16 [16, 384, 32, 1024], P(None, ('shot', 'gx'), 'gy', 'gz'), parts along dimension 1
The draws below stay inside these ranges and needn't reach their ends.
There are 2 independent parts, one for each index of `shot`. The reference program is written for one: setup_inputs(seed, part) draws one part's arguments, and reference() takes and returns one part's arrays. A program takes and returns all parts, laid end to end along the dimension named above; an argument that names none is the same for every part. Nothing has to cross between parts.
Inputs may be any that keep to these rules, and one draw needn't show every extreme that they name: `source_cell`: the source's cell as (x, y, z), each coordinate within the grid. `receiver_cells`: each row is a receiver's (x, y) within the grid, on the top surface at depth 0; several receivers may share a cell. Depth of a cell into the absorbing layers along the four side faces and the bottom face, largest at the grid's faces; 0 in the interior; the top face has no layer.
All inputs are finite; a program needn't handle non-finite values.
Results may differ from the reference program's by a relative error of at most 0.001.
Values sent between devices are 32-bit elements; how exact they have to be, the bound alone decides.
No kernel may reach another device: no remote copies, remote signals or barrier semaphores. Data moves between devices by JAX's collectives and lax.ppermute only.
A program may use at most 64 MiB of HBM per device.

```python
import math
import jax
import jax.numpy as jnp
from jax import lax

LAGS = 16
STEPS = 4
EVERY = 2
NX = 192
NY = 32
NZ = 1024
NREC = 2048


def draw_absorbing(key, part):
    sides = jax.random.randint(jax.random.fold_in(key, 11), (4,), 2, 9)
    x_cells = jnp.arange(NX, dtype=jnp.int32)
    y_cells = jnp.arange(NY, dtype=jnp.int32)
    z_cells = jnp.arange(NZ, dtype=jnp.int32)
    level_x = jnp.maximum(jnp.maximum(sides[0] - x_cells, sides[1] - (NX - 1 - x_cells)), 0)
    level_y = jnp.maximum(jnp.maximum(sides[2] - y_cells, sides[3] - (NY - 1 - y_cells)), 0)
    level_z = jnp.maximum(8 - (NZ - 1 - z_cells), 0)
    level = jnp.maximum(jnp.maximum(level_x[:, None, None], level_y[None, :, None]), level_z[None, None, :])
    return level.astype(jnp.int32)


def draw_source_cell(key, part):
    first = jax.random.randint(jax.random.fold_in(key, 21), (), 0, NX)
    second = jax.random.randint(jax.random.fold_in(key, 22), (), 0, NY)
    third = jax.random.randint(jax.random.fold_in(key, 23), (), 0, NZ)
    return jnp.stack([first, second, third]).astype(jnp.int32)


def draw_receiver_cells(key, part):
    first = jax.random.randint(jax.random.fold_in(key, 31), (NREC,), 0, NX)
    second = jax.random.randint(jax.random.fold_in(key, 32), (NREC,), 0, NY)
    return jnp.stack([first, second], axis=1).astype(jnp.int32)


def levels(key, shape, cuts, low, high):
    loudness, own = 1.0, jax.random.fold_in(key, 6)
    for dim, blocks in cuts:
        heights = jnp.exp(jax.random.uniform(jax.random.fold_in(own, dim), (blocks,), jnp.float32, low / len(cuts), high / len(cuts)))
        loudness = loudness * jnp.repeat(heights, shape[dim] // blocks).reshape([-1 if axis == dim else 1 for axis in range(len(shape))])
    return loudness


def bell_draw(rng, shape, spread, limit, split=(), kind=jnp.bfloat16):
    result = spread * jax.random.normal(rng, shape, jnp.float32)
    if split:
        result = result * levels(rng, shape, split, -0.22, 0.18)
    return jnp.clip(result, -limit, limit).astype(kind)


def setup_inputs(seed: int = 0, part: int = 0) -> dict:
    splits = jax.random.split(jax.random.key(seed), 11)
    part_keys = jax.random.split(jax.random.fold_in(splits[10], part), 11)
    return {
        "source_prev": bell_draw(part_keys[0], (NX, NY, NZ), 1.0, 6.0, ((0, 16), (1, 8), (2, 2)), jnp.float32),
        "source_now": bell_draw(part_keys[1], (NX, NY, NZ), 1.0, 6.0, ((0, 16), (1, 8), (2, 2)), jnp.float32),
        "receiver_prev": bell_draw(part_keys[2], (NX, NY, NZ), 1.0, 6.0, ((0, 16), (1, 8), (2, 2)), jnp.float32),
        "receiver_now": bell_draw(part_keys[3], (NX, NY, NZ), 1.0, 6.0, ((0, 16), (1, 8), (2, 2)), jnp.float32),
        "courant": jnp.clip(jnp.exp(math.log(0.16) - 1.3862944 * jax.random.uniform(splits[4], (NX, NY, NZ), jnp.float32) ** levels(splits[4], (NX, NY, NZ), ((0, 16), (1, 8), (2, 2)), -0.2, 0.2)), 0.04, 0.16),
        "absorbing": draw_absorbing(jax.random.fold_in(splits[10], 71), part),
        "source_cell": draw_source_cell(jax.random.fold_in(jax.random.fold_in(splits[10], part), 71), part),
        "wavelet": bell_draw(part_keys[7], (STEPS,), 1.0, 4.0, (), jnp.float32),
        "receiver_cells": draw_receiver_cells(jax.random.fold_in(jax.random.fold_in(splits[10], part), 71), part),
        "traces": bell_draw(part_keys[9], (STEPS, NREC), 1.0, 6.0, (), jnp.float32),
    }


stencil_weights = (8.0 / 5.0, -1.0 / 5.0, 8.0 / 315.0, -1.0 / 560.0)
centre_weight = -205.0 / 72.0


def stencil(padded):
    size_x = padded.shape[-3] - 8
    size_y = padded.shape[-2] - 8
    size_z = padded.shape[-1] - 8

    def window(start_x, start_y, start_z):
        return padded[..., start_x:start_x + size_x, start_y:start_y + size_y, start_z:start_z + size_z]

    total = (3.0 * centre_weight) * window(4, 4, 4)
    for reach, weight in enumerate(stencil_weights, 1):
        total = total + weight * (window(4 + reach, 4, 4) + window(4 - reach, 4, 4) + window(4, 4 + reach, 4) + window(4, 4 - reach, 4) + window(4, 4, 4 + reach) + window(4, 4, 4 - reach))
    return total


def advance(padded, current, earlier, courant, damping):
    return (2.0 * current - (1.0 - damping) * earlier + courant * stencil(padded)) / (1.0 + damping)


def laplace(padded):
    size_x = padded.shape[-3] - 2
    size_y = padded.shape[-2] - 2
    size_z = padded.shape[-1] - 2

    def window(start_x, start_y, start_z):
        return padded[..., start_x:start_x + size_x, start_y:start_y + size_y, start_z:start_z + size_z]

    return 6.0 * window(1, 1, 1) - (window(2, 1, 1) + window(0, 1, 1) + window(1, 2, 1) + window(1, 0, 1) + window(1, 1, 2) + window(1, 1, 0))


def reference(source_prev, source_now, receiver_prev, receiver_now, courant, absorbing, source_cell, wavelet, receiver_cells, traces):
    earlier = jnp.stack([source_prev, receiver_prev])
    current = jnp.stack([source_now, receiver_now])
    damping = absorbing.astype(jnp.float32) / 16.0
    snapshots = []
    for step_index in range(STEPS):
        padded = jnp.pad(current, ((0, 0), (4, 4), (4, 4), (4, 4)))
        upcoming = advance(padded, current, earlier, courant, damping)
        upcoming = upcoming.at[0, source_cell[0], source_cell[1], source_cell[2]].add(wavelet[step_index])
        upcoming = upcoming.at[1, receiver_cells[:, 0], receiver_cells[:, 1], 0].add(traces[step_index])
        earlier, current = current, upcoming
        if (step_index + 1) % EVERY == 0:
            snapshots.append(jnp.pad(current, ((0, 0), (LAGS // 2, LAGS // 2), (0, 0), (0, 0))))

    def one_lag(offset):
        image = jnp.zeros((NX, NY, NZ), jnp.float32)
        for widened in snapshots:
            image = image + lax.dynamic_slice_in_dim(widened[0], (LAGS - offset).astype(jnp.int32), NX, 0) * lax.dynamic_slice_in_dim(widened[1], offset.astype(jnp.int32), NX, 0)
        return laplace(jnp.pad(image, 1)).astype(jnp.bfloat16)

    filtered_image = lax.map(one_lag, jnp.arange(LAGS, dtype=jnp.int32))
    return current[0], current[1], filtered_image
```

```python
import jax
import jax.numpy as jnp
from jax import lax
from jax.sharding import PartitionSpec as P

LAGS = 16
STEPS = 4
EVERY = 2


stencil_weights = (8.0 / 5.0, -1.0 / 5.0, 8.0 / 315.0, -1.0 / 560.0)
centre_weight = -205.0 / 72.0


def edges_of(array, axis, dim, width):
    size, here, length = (lax.axis_size(axis), lax.axis_index(axis), array.shape[dim])
    last = lax.slice_in_dim(array, length - width, length, axis=dim)
    first = lax.slice_in_dim(array, 0, width, axis=dim)
    if size == 2:
        other = lax.ppermute(jnp.where(here == 0, last, first), axis, [(0, 1), (1, 0)])
        before = after = other
    else:
        up = [(i, (i + 1) % size) for i in range(size)]
        before = lax.ppermute(last, axis, up)
        after = lax.ppermute(first, axis, [(b, a) for a, b in up])
    return (jnp.where(here > 0, before, 0.0), jnp.where(here < size - 1, after, 0.0))


def with_halo(array, sides, width):
    for axis, dim in sides:
        before, after = edges_of(array, axis, dim, width)
        array = jnp.concatenate([before, array, after], axis=dim)
    return array


def extended(array, sides, width):
    edges = {dim: edges_of(array, axis, dim, width) for axis, dim in sides}
    done = []
    for _, dim in sides:
        low, high = edges[dim]
        around = [(width, width) if d in done else (0, 0) for d in range(array.ndim)]
        array = jnp.concatenate([jnp.pad(low, around), array, jnp.pad(high, around)], axis=dim)
        done.append(dim)
    return array


def stencil(padded):
    size_x = padded.shape[-3] - 8
    size_y = padded.shape[-2] - 8
    size_z = padded.shape[-1] - 8

    def window(start_x, start_y, start_z):
        return padded[
            ..., start_x : start_x + size_x, start_y : start_y + size_y, start_z : start_z + size_z
        ]

    total = 3.0 * centre_weight * window(4, 4, 4)
    for reach, weight in enumerate(stencil_weights, 1):
        total = total + weight * (
            window(4 + reach, 4, 4)
            + window(4 - reach, 4, 4)
            + window(4, 4 + reach, 4)
            + window(4, 4 - reach, 4)
            + window(4, 4, 4 + reach)
            + window(4, 4, 4 - reach)
        )
    return total


def advance(padded, current, earlier, courant, damping):
    return (2.0 * current - (1.0 - damping) * earlier + courant * stencil(padded)) / (1.0 + damping)


def laplace(padded):
    size_x = padded.shape[-3] - 2
    size_y = padded.shape[-2] - 2
    size_z = padded.shape[-1] - 2

    def window(start_x, start_y, start_z):
        return padded[
            ..., start_x : start_x + size_x, start_y : start_y + size_y, start_z : start_z + size_z
        ]

    return 6.0 * window(1, 1, 1) - (
        window(2, 1, 1)
        + window(0, 1, 1)
        + window(1, 2, 1)
        + window(1, 0, 1)
        + window(1, 1, 2)
        + window(1, 1, 0)
    )


def correlate(widened, length):
    return jnp.stack(
        [
            widened[0, LAGS - offset : LAGS - offset + length]
            * widened[1, offset : offset + length]
            for offset in range(LAGS)
        ]
    )


def local(
    source_prev,
    source_now,
    receiver_prev,
    receiver_now,
    courant,
    absorbing,
    source_cell,
    wavelet,
    receiver_cells,
    traces,
):
    earlier = jnp.stack([source_prev, receiver_prev])
    current = jnp.stack([source_now, receiver_now])
    damping = absorbing.astype(jnp.float32) / 16.0
    tile_x, tile_y, tile_z = courant.shape
    x_anchor = lax.axis_index("gx") * tile_x
    y_cells = jnp.arange(tile_y, dtype=jnp.int32) + lax.axis_index("gy") * tile_y
    z_cells = jnp.arange(tile_z, dtype=jnp.int32) + lax.axis_index("gz") * tile_z
    surface = (lax.axis_index("gz") == 0).astype(jnp.float32)
    image = None
    x_cells = jnp.arange(tile_x, dtype=jnp.int32) + x_anchor
    for step_index in range(STEPS):
        padded = extended(current, (("gx", 1), ("gy", 2), ("gz", 3)), 4)
        upcoming = advance(padded, current, earlier, courant, damping)
        inject_upcoming = upcoming
        hit_x = (x_cells == source_cell[0]).astype(jnp.float32)
        hit_y = (y_cells == source_cell[1]).astype(jnp.float32)
        hit_z = (z_cells == source_cell[2]).astype(jnp.float32)
        point = hit_x[:, None, None] * hit_y[None, :, None] * hit_z[None, None, :]
        match_x = (receiver_cells[:, 0:1] == x_cells[None, :]).astype(jnp.float32) * traces[
            step_index
        ][:, None]
        match_y = (receiver_cells[:, 1:2] == y_cells[None, :]).astype(jnp.float32)
        sheet = jnp.einsum("rx,ry->xy", match_x, match_y, precision=lax.Precision.HIGHEST) * surface
        inject_upcoming = inject_upcoming.at[0].add(point * wavelet[step_index])
        upcoming = inject_upcoming.at[1, :, :, 0].add(sheet)
        earlier, current = (current, upcoming)
        if (step_index + 1) % EVERY == 0:
            widened = with_halo(current, (("gx", 1),), LAGS // 2)
            term = correlate(widened, tile_x)
            image = term if image is None else image + term
    framed = extended(image, (("gx", 1), ("gy", 2), ("gz", 3)), 1)
    filtered_image = laplace(framed).astype(jnp.bfloat16)
    return (current[0], current[1], filtered_image)


def solution(mesh):
    placed = (
        P(("shot", "gx"), "gy", "gz"),
        P(("shot", "gx"), "gy", "gz"),
        P(("shot", "gx"), "gy", "gz"),
        P(("shot", "gx"), "gy", "gz"),
        P("gx", "gy", "gz"),
        P("gx", "gy", "gz"),
        P("shot"),
        P("shot"),
        P("shot", None),
        P(None, "shot"),
    )
    return jax.shard_map(
        local,
        mesh=mesh,
        in_specs=placed,
        out_specs=(
            P(("shot", "gx"), "gy", "gz"),
            P(("shot", "gx"), "gy", "gz"),
            P(None, ("shot", "gx"), "gy", "gz"),
        ),
        check_vma=False,
    )
```

```python
import functools

import jax
import jax.numpy as jnp
from jax import lax
from jax.experimental import pallas as pl
from jax.experimental.pallas import tpu as pltpu
from jax.sharding import PartitionSpec as P

LAGS = 16
STEPS = 4
EVERY = 2
LANES = 128
HALF = LAGS // 2
WIDE = HALF + 1

stencil_weights = (8.0 / 5.0, -1.0 / 5.0, 8.0 / 315.0, -1.0 / 560.0)
centre_weight = -205.0 / 72.0


def pairs(size):
    near = [(i, i ^ 1) for i in range(size)]
    far = [(i, (i + 1) % size if i % 2 else (i - 1) % size) for i in range(size)]
    return near, far


def swap(a, b, axis):
    near, far = pairs(lax.axis_size(axis))
    return lax.ppermute(a, axis, near), lax.ppermute(b, axis, far)


def cross(a):
    return lax.ppermute(a, "gz", [(0, 1), (1, 0)])


def rows():
    return lax.broadcasted_iota(jnp.int32, (8, LANES), 0)


def lanes():
    return lax.broadcasted_iota(jnp.int32, (8, LANES), 1)


def place(axis):
    index = lax.axis_index(axis)
    return index, lax.rem(index, 2) == 1, index > 0, index < lax.axis_size(axis) - 1


def chunk(j):
    return slice(j * LANES, (j + 1) * LANES)


def kept(flag, value):
    return jnp.where(flag, value, jnp.zeros_like(value))


def call(body, outs, *args, scratch=(), smem=(), far=(), far_outs=()):
    args = [
        a if i in far or i in smem else pltpu.with_memory_space_constraint(a, pltpu.VMEM)
        for i, a in enumerate(args)
    ]
    return pl.pallas_call(
        body,
        out_shape=[
            jax.ShapeDtypeStruct(s, d) if i in far_outs else pltpu.VMEM(s, d)
            for i, (s, d) in enumerate(outs)
        ],
        in_specs=[
            pl.BlockSpec(memory_space=pltpu.SMEM if i in smem else pltpu.VMEM)
            for i in range(len(args))
        ],
        out_specs=[pl.BlockSpec(memory_space=pltpu.VMEM)] * len(outs),
        scratch_shapes=list(scratch),
        compiler_params=pltpu.CompilerParams(vmem_limit_bytes=8 * 2**20),
        name=body.func.__name__ if isinstance(body, functools.partial) else body.__name__,
    )(*args)


def put_sides(tile, a_ref, b_ref, width):
    odd = place("gx")[1]
    size = tile.shape[0]
    for k in range(width):
        low, high = tile[k], tile[size - width + k]
        a_ref[k] = jnp.where(odd, low, high)
        b_ref[k] = jnp.where(odd, high, low)


def put_edge(tile, z_ref, at=0):
    last = place("gz")[0] == 0
    for k in range(tile.shape[0]):
        z_ref[at + k] = jnp.where(last, tile[k, :, -LANES:], tile[k, :, :LANES])


def pack(source, receiver, tile, a_ref, b_ref, z_ref):
    for k in range(tile.shape[0]):
        tile[k, 0:4] = source[k]
        tile[k, 4:8] = receiver[k]
    put_sides(tile, a_ref, b_ref, 4)
    put_edge(tile, z_ref)


def prepare(cell, wavelet, spots, traces, courant, absorbing, source, receiver, coef, before, inject, code_ref, amp_ref):
    size_x, size_y, size_z = courant.shape
    for k in range(size_x):
        before[k, 0:4] = source[k]
        before[k, 4:8] = receiver[k]
        damping = absorbing[k].astype(jnp.float32) / 16.0
        inverse = 1.0 / (1.0 + damping)
        for half in (slice(0, 4), slice(4, 8)):
            coef[0, k, half] = 2.0 * inverse
            coef[1, k, half] = (1.0 - damping) * inverse
            coef[2, k, half] = courant[k] * inverse
    gx, gy, gz = (lax.axis_index(a) for a in ("gx", "gy", "gz"))
    sx, sy, sz = cell[0] - gx * size_x, cell[1] - gy * size_y, cell[2] - gz * size_z
    at_x, at_y = spots[0:1] - gx * size_x, spots[1:2] - gy * size_y
    inside = (at_x >= 0) & (at_x < size_x) & (at_y >= 0) & (at_y < size_y) & (gz == 0)
    code = jnp.where(inside, at_x * 8 + at_y + 4, -1)
    blocks = code.shape[1] // LANES
    for b in range(blocks):
        code_ref[b] = jnp.broadcast_to(code[:, chunk(b)], (8, LANES))
        for t in range(STEPS):
            amp_ref[t, b] = jnp.broadcast_to(traces[t : t + 1, chunk(b)], (8, LANES))
    row, lane = rows(), lanes()

    def each(k, carry):
        sums = [jnp.zeros((8, LANES), jnp.float32) for _ in range(STEPS)]
        for b in range(blocks):
            hit = code_ref[b] == row + k * 8
            for t in range(STEPS):
                sums[t] = sums[t] + jnp.where(hit, amp_ref[t, b], 0.0)
        for t in range(STEPS):
            sheet = jnp.where(lane == 0, jnp.sum(sums[t], axis=1, keepdims=True), 0.0)
            for j in range(size_z // LANES):
                spot = (row == sy) & (sy < 4) & (lane + j * LANES == sz) & (k == sx)
                point = jnp.where(spot, wavelet[t], 0.0)
                inject[t, k, :, chunk(j)] = point + sheet if j == 0 else point
        return carry

    lax.fori_loop(0, size_x, each, 0)


def forward(step, cur, prev, coef, inject, xa, xb, ya, yb, z, new):
    size_x, _, size_z = cur.shape
    count = size_z // LANES
    _, odd_x, below_x, above_x = place("gx")
    _, odd_y, below_y, above_y = place("gy")
    first = lax.axis_index("gz") == 0
    wide = xa.shape[0] if step == 2 else 4
    row, lane = lax.rem(rows(), 4), lanes()

    def at(x, j):
        if x < 0:
            return kept(below_x, jnp.where(odd_x, xa[wide + x, :, chunk(j)], xb[wide + x, :, chunk(j)]))
        if x >= size_x:
            return kept(above_x, jnp.where(odd_x, xb[x - size_x, :, chunk(j)], xa[x - size_x, :, chunk(j)]))
        return cur[x, :, chunk(j)]

    for x in range(size_x):
        own = [cur[x, :, chunk(j)] for j in range(count)]
        beyond = z[x]
        before, after = kept(jnp.logical_not(first), beyond), kept(first, beyond)
        along = [None] * count
        for k, weight in enumerate(stencil_weights, 1):
            up = [pltpu.roll(v, LANES - k, axis=1) for v in (*own, after)]
            down = [pltpu.roll(v, k, axis=1) for v in (before, *own)]
            for j in range(count):
                both = jnp.where(lane < LANES - k, up[j], up[j + 1]) + jnp.where(lane >= k, down[j + 1], down[j])
                both = both + at(x + k, j) + at(x - k, j)
                along[j] = weight * both if along[j] is None else along[j] + weight * both
        for j in range(count):
            s = chunk(j)
            centre = own[j]
            low = kept(below_y, jnp.where(odd_y, ya[x, :, s], yb[x, :, s]))
            high = kept(above_y, jnp.where(odd_y, yb[x, :, s], ya[x, :, s]))
            total = 3.0 * centre_weight * centre + along[j] + stencil_weights[3] * (low + high)
            for k, weight in enumerate(stencil_weights[:3], 1):
                up = jnp.where(row < 4 - k, pltpu.roll(centre, 8 - k, axis=0), pltpu.roll(high, 4 - k, axis=0))
                down = jnp.where(row >= k, pltpu.roll(centre, k, axis=0), pltpu.roll(low, 4 + k, axis=0))
                total = total + weight * (up + down)
            new[x, :, s] = (
                coef[0, x, :, s] * centre - coef[1, x, :, s] * prev[x, :, s] + coef[2, x, :, s] * total
            ) + inject[step, x, :, s]


def margin(ya, yb, x, s, row):
    _, odd, below, above = place("gy")
    low = kept(below, jnp.where(odd, ya[x, :, s], yb[x, :, s]))
    high = kept(above, jnp.where(odd, yb[x, :, s], ya[x, :, s]))
    return jnp.where(lax.rem(row, 4) == 0, high, low)


def put_margins(get, size_x, count, a_ref, b_ref, at):
    odd = place("gx")[1]
    row = rows()
    outer = (lax.rem(row, 4) == 0) | (lax.rem(row, 4) == 3)
    for i in range((WIDE + 1) // 2):
        for j in range(count):
            sides = []
            for start in (0, size_x - WIDE):
                one = get(start + 2 * i, j)
                if 2 * i + 1 < WIDE:
                    one = jnp.where(outer, one, pltpu.roll(get(start + 2 * i + 1, j), 2, axis=0))
                sides.append(one)
            a_ref[at + i, :, chunk(j)] = jnp.where(odd, sides[0], sides[1])
            b_ref[at + i, :, chunk(j)] = jnp.where(odd, sides[1], sides[0])


def around_x(x, s, cur, xa, xb):
    _, odd, below, above = place("gx")
    size_x = cur.shape[0]
    if x < 0:
        return kept(below, jnp.where(odd, xa[WIDE + x, :, s], xb[WIDE + x, :, s]))
    if x >= size_x:
        return kept(above, jnp.where(odd, xb[x - size_x, :, s], xa[x - size_x, :, s]))
    return cur[x, :, s]


def first_step(cur, prev, coef, inject, xa, xb, ya, yb, z, new, a_ref, b_ref, z_ref):
    forward(0, cur, prev, coef, inject, xa, xb, ya, yb, z, new)
    put_sides(new, a_ref, b_ref, 4)
    put_edge(new, z_ref)


def second_step(cur, prev, coef, inject, xa, xb, ya, yb, z, new, a_ref, b_ref, z_ref):
    forward(1, cur, prev, coef, inject, xa, xb, ya, yb, z, new)
    put_sides(new, a_ref, b_ref, WIDE)
    put_edge(new, z_ref)


def put_wide_edge(cur, xa, xb, z_ref, at):
    size_x, _, size_z = cur.shape
    last = lax.axis_index("gz") == 0
    for x in range(-WIDE, size_x + WIDE):
        ends = [around_x(x, s, cur, xa, xb) for s in (slice(size_z - LANES, size_z), slice(0, LANES))]
        z_ref[at + WIDE + x] = jnp.where(last, ends[0], ends[1])


def third_step(cur, prev, coef, inject, xa, xb, ya, yb, z, new, a_ref, b_ref, z_ref):
    forward(2, cur, prev, coef, inject, xa, xb, ya, yb, z, new)
    size_x, _, size_z = cur.shape
    put_sides(new, a_ref, b_ref, 4)
    row = rows()
    put_margins(lambda x, j: margin(ya, yb, x, chunk(j), row), size_x, size_z // LANES, a_ref, b_ref, 4)
    put_edge(new, z_ref)
    put_wide_edge(cur, xa, xb, z_ref, size_x)


def fourth_step(cur, prev, coef, inject, xa, xb, ya, yb, z, new, source, receiver, a_ref, b_ref, ya_ref, yb_ref):
    forward(3, cur, prev, coef, inject, xa, xb, ya, yb, z, new)
    size_x, _, size_z = cur.shape
    put_sides(new, a_ref, b_ref, WIDE)
    odd = place("gy")[1]
    row = lax.rem(rows(), 4)
    for x in range(size_x):
        source[x] = new[x, 0:4]
        receiver[x] = new[x, 4:8]
    for i in range(size_x // 4):
        for j in range(size_z // LANES):
            tops, bottoms = [], []
            for q in range(4):
                value = new[4 * i + q, :, chunk(j)]
                tops.append(value if q == 0 else pltpu.roll(value, 8 - q, axis=0))
                bottoms.append(pltpu.roll(value, 3 - q, axis=0) if q < 3 else value)
            high, low = tops[0], bottoms[0]
            for q in range(1, 4):
                high = jnp.where(row == 3 - q, tops[q], high)
                low = jnp.where(row == 3 - q, bottoms[q], low)
            ya_ref[i, :, chunk(j)] = jnp.where(odd, low, high)
            yb_ref[i, :, chunk(j)] = jnp.where(odd, high, low)


def gather_edges(cur, xa, xb, ya, yb, margins, a_ref, b_ref, z_ref):
    size_x, _, size_z = cur.shape
    _, odd, below, above = place("gy")
    row = lax.rem(rows(), 4)
    for x in range(size_x):
        i, q = divmod(x, 4)
        for j in range(size_z // LANES):
            s = chunk(j)
            low = kept(below, jnp.where(odd, ya[i, :, s], yb[i, :, s]))
            high = kept(above, jnp.where(odd, yb[i, :, s], ya[i, :, s]))
            if q:
                low = pltpu.roll(low, q, axis=0)
            high = pltpu.roll(high, (q + 5) % 8, axis=0)
            margins[x, :, s] = jnp.where(row == 0, high, low)
    put_margins(lambda x, j: margins[x, :, chunk(j)], size_x, size_z // LANES, a_ref, b_ref, 0)
    put_wide_edge(cur, xa, xb, z_ref, 0)


def widen(get_margin, cur, xa, xb, ma, mb, m_at, zw, z_at, first_ref, second_ref, first_z, second_z):
    size_x, _, size_z = cur.shape
    _, odd, below, above = place("gx")
    row = rows()
    own = row < 4
    for x in range(-WIDE, size_x + WIDE):
        e = x + WIDE
        for j in range(size_z // LANES):
            s = chunk(j)
            if 0 <= x < size_x:
                edge = get_margin(x, s)
            else:
                k = e if x < 0 else x - size_x
                i, other = divmod(k, 2)
                near, far = ma[m_at + i, :, s], mb[m_at + i, :, s]
                edge = kept(below, jnp.where(odd, near, far)) if x < 0 else kept(above, jnp.where(odd, far, near))
                if other:
                    edge = pltpu.roll(edge, 6, axis=0)
            both = around_x(x, s, cur, xa, xb)
            first_ref[e, :, s] = jnp.where(own, both, pltpu.roll(edge, 4, axis=0))
            second_ref[e, :, s] = jnp.where(own, pltpu.roll(both, 4, axis=0), edge)
        first_z[e] = zw[z_at + e]
        second_z[e] = pltpu.roll(zw[z_at + e], 4, axis=0)


def early(cur, xa, xb, ya, yb, ma, mb, zw, first_ref, second_ref, first_z, second_z):
    row = rows()
    widen(
        lambda x, s: margin(ya, yb, x, s, row), cur, xa, xb, ma, mb, 4, zw, cur.shape[0],
        first_ref, second_ref, first_z, second_z,
    )


def filtered(s2, r2, s2z, r2z, cur, margins, xa, xb, ma, mb, zw, out, s4, r4, s4z, r4z):
    size_x, _, size_z = cur.shape
    count = size_z // LANES
    widen(lambda x, s: margins[x, :, s], cur, xa, xb, ma, mb, 0, zw, 0, s4, r4, s4z, r4z)
    first = lax.axis_index("gz") == 0
    lane = lanes()

    def each(lag, carry):
        def image(x):
            a, b = x - lag + HALF + WIDE, x + lag - HALF + WIDE
            return [
                s2[a, :, chunk(j)] * r2[b, :, chunk(j)] + s4[a, :, chunk(j)] * r4[b, :, chunk(j)]
                for j in range(count)
            ]

        previous, here = image(-1), image(0)
        for x in range(size_x):
            following = image(x + 1)
            a, b = x - lag + HALF + WIDE, x + lag - HALF + WIDE
            beyond = s2z[a] * r2z[b] + s4z[a] * r4z[b]
            before, after = kept(jnp.logical_not(first), beyond), kept(first, beyond)
            up = [pltpu.roll(v, LANES - 1, axis=1) for v in (*here, after)]
            down = [pltpu.roll(v, 1, axis=1) for v in (before, *here)]
            for j in range(count):
                along = jnp.where(lane < LANES - 1, up[j], up[j + 1]) + jnp.where(lane >= 1, down[j + 1], down[j])
                across = pltpu.roll(here[j], 7, axis=0) + pltpu.roll(here[j], 1, axis=0)
                value = 6.0 * here[j] - (previous[j] + following[j] + across + along)
                out[lag, x, :, chunk(j)] = value[0:4].astype(jnp.bfloat16)
            previous, here = here, following
        return carry

    lax.fori_loop(0, LAGS, each, 0)


def local(
    source_prev,
    source_now,
    receiver_prev,
    receiver_now,
    courant,
    absorbing,
    source_cell,
    wavelet,
    receiver_cells,
    traces,
):
    f32 = jnp.float32
    size_x, size_y, size_z = courant.shape
    tile = ((size_x, 8, size_z), f32)
    wide_x = size_x + 2 * WIDE
    packed = (WIDE + 1) // 2

    def side(n):
        return ((n, 8, size_z), f32)

    def edge(n):
        return ((n, 8, LANES), f32)

    now, a, b, z = call(pack, [tile, side(4), side(4), edge(size_x)], source_now, receiver_now, far=(0, 1))
    halo0 = (*swap(a, b, "gx"), *swap(now, now, "gy"), cross(z))
    blocks = receiver_cells.shape[0] // LANES
    coef, prev, inject = call(
        prepare,
        [((3, *tile[0]), f32), tile, ((STEPS, *tile[0]), f32)],
        source_cell, wavelet, receiver_cells.T, traces, courant, absorbing, source_prev, receiver_prev,
        scratch=[pltpu.VMEM((blocks, 8, LANES), jnp.int32), pltpu.VMEM((STEPS, blocks, 8, LANES), f32)],
        smem=(0, 1),
        far=range(8),
    )
    one, a, b, z = call(first_step, [tile, side(4), side(4), edge(size_x)], now, prev, coef, inject, *halo0)
    halo1 = (*swap(a, b, "gx"), *swap(one, one, "gy"), cross(z))
    two, a, b, z = call(second_step, [tile, side(WIDE), side(WIDE), edge(size_x)], one, now, coef, inject, *halo1)
    halo2 = (*swap(a, b, "gx"), *swap(two, two, "gy"), cross(z))
    three, a, b, z = call(
        third_step,
        [tile, side(4 + packed), side(4 + packed), edge(size_x + wide_x)],
        two, one, coef, inject, *halo2,
    )
    halo3 = (*swap(a, b, "gx"), *swap(three, three, "gy"), cross(z))
    field = ((size_x, size_y, size_z), f32)
    four, source, receiver, a, b, c, d = call(
        fourth_step,
        [tile, field, field, side(WIDE), side(WIDE), side(size_x // 4), side(size_x // 4)],
        three, two, coef, inject, *halo3,
        far_outs=(1, 2),
    )
    halo4 = (*swap(a, b, "gx"), *swap(c, d, "gy"))
    s2, r2, s2z, r2z = call(
        early,
        [side(wide_x), side(wide_x), edge(wide_x), edge(wide_x)],
        two, *halo2[:4], halo3[0], halo3[1], halo3[4],
    )
    margins, a, b, z = call(
        gather_edges, [tile, side(packed), side(packed), edge(wide_x)], four, *halo4
    )
    halo5 = (*swap(a, b, "gx"), cross(z))
    (image,) = call(
        filtered,
        [((LAGS, size_x, size_y, size_z), jnp.bfloat16)],
        s2, r2, s2z, r2z, four, margins, halo4[0], halo4[1], *halo5,
        scratch=[pltpu.VMEM(s, f32) for s, _ in (side(wide_x), side(wide_x), edge(wide_x), edge(wide_x))],
        far_outs=(0,),
    )
    return source, receiver, image


def solution(mesh):
    placed = (
        P(("shot", "gx"), "gy", "gz"),
        P(("shot", "gx"), "gy", "gz"),
        P(("shot", "gx"), "gy", "gz"),
        P(("shot", "gx"), "gy", "gz"),
        P("gx", "gy", "gz"),
        P("gx", "gy", "gz"),
        P("shot"),
        P("shot"),
        P("shot", None),
        P(None, "shot"),
    )
    return jax.shard_map(
        local,
        mesh=mesh,
        in_specs=placed,
        out_specs=(
            P(("shot", "gx"), "gy", "gz"),
            P(("shot", "gx"), "gy", "gz"),
            P(None, ("shot", "gx"), "gy", "gz"),
        ),
        check_vma=False,
    )
```

```python
import functools

import jax
import jax.numpy as jnp
from jax import lax
from jax.experimental import pallas as pl
from jax.experimental.pallas import tpu as pltpu
from jax.sharding import PartitionSpec as P

LAGS = 16
STEPS = 4
EVERY = 2
LANES = 128
HALF = LAGS // 2
WIDE = HALF + 1

stencil_weights = (8.0 / 5.0, -1.0 / 5.0, 8.0 / 315.0, -1.0 / 560.0)
centre_weight = -205.0 / 72.0


def pairs(size):
    near = [(i, i ^ 1) for i in range(size)]
    far = [(i, (i + 1) % size if i % 2 else (i - 1) % size) for i in range(size)]
    return near, far


def swap(a, b, axis):
    near, far = pairs(lax.axis_size(axis))
    return lax.ppermute(a, axis, near), lax.ppermute(b, axis, far)


def cross(a):
    return lax.ppermute(a, "gz", [(0, 1), (1, 0)])


def rows():
    return lax.broadcasted_iota(jnp.int32, (8, LANES), 0)


def lanes():
    return lax.broadcasted_iota(jnp.int32, (8, LANES), 1)


def place(axis):
    index = lax.axis_index(axis)
    return index, lax.rem(index, 2) == 1, index > 0, index < lax.axis_size(axis) - 1


def chunk(j):
    return slice(j * LANES, (j + 1) * LANES)


def kept(flag, value):
    return jnp.where(flag, value, jnp.zeros_like(value))


def call(body, outs, *args, scratch=(), smem=(), far=(), far_outs=()):
    args = [
        a if i in smem else pltpu.with_memory_space_constraint(a, pltpu.HBM if i in far else pltpu.VMEM)
        for i, a in enumerate(args)
    ]
    return pl.pallas_call(
        body,
        out_shape=[
            jax.ShapeDtypeStruct(s, d) if i in far_outs else pltpu.VMEM(s, d)
            for i, (s, d) in enumerate(outs)
        ],
        in_specs=[
            pl.BlockSpec(memory_space=pltpu.SMEM if i in smem else pltpu.VMEM)
            for i in range(len(args))
        ],
        out_specs=[pl.BlockSpec(memory_space=pltpu.VMEM)] * len(outs),
        scratch_shapes=list(scratch),
        compiler_params=pltpu.CompilerParams(vmem_limit_bytes=8 * 2**20),
        name=body.func.__name__ if isinstance(body, functools.partial) else body.__name__,
    )(*args)


def put_sides(tile, a_ref, b_ref, width):
    odd = place("gx")[1]
    size = tile.shape[0]
    for k in range(width):
        low, high = tile[k], tile[size - width + k]
        a_ref[k] = jnp.where(odd, low, high)
        b_ref[k] = jnp.where(odd, high, low)


def merge(source, receiver, before, behind, courant, absorbing, now, prev, medium, z_ref):
    last = place("gz")[0] == 0
    size_x, _, size_z = source.shape
    for k in range(size_x):
        now[k, 0:4] = source[k]
        now[k, 4:8] = receiver[k]
        prev[k, 0:4] = before[k]
        prev[k, 4:8] = behind[k]
        medium[k, 0:4] = courant[k]
        medium[k, 4:8] = absorbing[k].astype(jnp.float32)
    for n, tile in enumerate((now, prev, medium)):
        for k in range(size_x):
            z_ref[n * size_x + k] = jnp.where(last, tile[k, :, -LANES:], tile[k, :, :LANES])


def pack(now, beyond, tile, a_ref, b_ref):
    size_x, _, size_z = now.shape
    for k in range(size_x):
        tile[k, :, :size_z] = now[k]
        tile[k, :, size_z:] = beyond[k]
    put_sides(tile, a_ref, b_ref, 4)


def prepare(cell, wavelet, spots, traces, old, medium, beyond, coef, prev, inject, code_ref, amp_ref):
    size_x, _, size_z = old.shape
    first = lax.axis_index("gz") == 0
    count = size_z // LANES
    for k in range(size_x):
        prev[k, :, :size_z] = old[k]
        prev[k, :, size_z:] = beyond[size_x + k]
        for j in range(count + 1):
            both = medium[k, :, chunk(j)] if j < count else beyond[2 * size_x + k]
            upper = rows() < 4
            turned = pltpu.roll(both, 4, axis=0)
            courant = jnp.where(upper, both, turned)
            damping = jnp.where(upper, turned, both) / 16.0
            inverse = 1.0 / (1.0 + damping)
            coef[0, k, :, chunk(j)] = 2.0 * inverse
            coef[1, k, :, chunk(j)] = (1.0 - damping) * inverse
            coef[2, k, :, chunk(j)] = courant * inverse
    gx, gy, gz = (lax.axis_index(a) for a in ("gx", "gy", "gz"))
    sx, sy, sz = cell[0] - gx * size_x, cell[1] - gy * 4, cell[2] - gz * size_z
    at_x, at_y = spots[0:1] - gx * size_x, spots[1:2] - gy * 4
    inside = (at_x >= 0) & (at_x < size_x) & (at_y >= 0) & (at_y < 4) & (gz == 0)
    code = jnp.where(inside, at_x * 8 + at_y + 4, -1)
    blocks = code.shape[1] // LANES
    for b in range(blocks):
        code_ref[b] = jnp.broadcast_to(code[:, chunk(b)], (8, LANES))
        for t in range(STEPS):
            amp_ref[t, b] = jnp.broadcast_to(traces[t : t + 1, chunk(b)], (8, LANES))
    row, lane = rows(), lanes()

    def each(k, carry):
        sums = [jnp.zeros((8, LANES), jnp.float32) for _ in range(STEPS)]
        for b in range(blocks):
            hit = code_ref[b] == row + k * 8
            for t in range(STEPS):
                sums[t] = sums[t] + jnp.where(hit, amp_ref[t, b], 0.0)
        for t in range(STEPS):
            sheet = jnp.where(lane == 0, jnp.sum(sums[t], axis=1, keepdims=True), 0.0)
            for j in range(count + 1):
                start = j * LANES if j < count else jnp.where(first, size_z, -LANES)
                spot = (row == sy) & (sy < 4) & (lane + start == sz) & (k == sx)
                point = jnp.where(spot, wavelet[t], 0.0)
                inject[t, k, :, chunk(j)] = point + sheet if j == 0 else point
        return carry

    lax.fori_loop(0, size_x, each, 0)


def forward(step, cur, prev, coef, inject, xa, xb, ya, yb, new):
    size_x, _, size_z = cur.shape
    count = size_z // LANES
    _, odd_x, below_x, above_x = place("gx")
    _, odd_y, below_y, above_y = place("gy")
    first = lax.axis_index("gz") == 0
    second = jnp.logical_not(first)
    wide = xa.shape[0] if step == 2 else 4
    row, lane = lax.rem(rows(), 4), lanes()

    def at(x, j):
        if x < 0:
            return kept(below_x, jnp.where(odd_x, xa[wide + x, :, chunk(j)], xb[wide + x, :, chunk(j)]))
        if x >= size_x:
            return kept(above_x, jnp.where(odd_x, xb[x - size_x, :, chunk(j)], xa[x - size_x, :, chunk(j)]))
        return cur[x, :, chunk(j)]

    for x in range(size_x):
        own = [cur[x, :, chunk(j)] for j in range(count)]
        along = [None] * count
        for k, weight in enumerate(stencil_weights, 1):
            up = [pltpu.roll(v, LANES - k, axis=1) for v in own]
            down = [pltpu.roll(v, k, axis=1) for v in own]
            after = [*up[1 : count - 1], kept(first, up[count - 1]), kept(second, up[0])]
            before = [kept(second, down[count - 1]), *down[: count - 2], kept(first, down[count - 2])]
            for j in range(count):
                both = jnp.where(lane < LANES - k, up[j], after[j]) + jnp.where(lane >= k, down[j], before[j])
                both = both + at(x + k, j) + at(x - k, j)
                along[j] = weight * both if along[j] is None else along[j] + weight * both
        for j in range(count):
            s = chunk(j)
            centre = own[j]
            low = kept(below_y, jnp.where(odd_y, ya[x, :, s], yb[x, :, s]))
            high = kept(above_y, jnp.where(odd_y, yb[x, :, s], ya[x, :, s]))
            total = 3.0 * centre_weight * centre + along[j] + stencil_weights[3] * (low + high)
            for k, weight in enumerate(stencil_weights[:3], 1):
                up = jnp.where(row < 4 - k, pltpu.roll(centre, 8 - k, axis=0), pltpu.roll(high, 4 - k, axis=0))
                down = jnp.where(row >= k, pltpu.roll(centre, k, axis=0), pltpu.roll(low, 4 + k, axis=0))
                total = total + weight * (up + down)
            new[x, :, s] = (
                coef[0, x, :, s] * centre - coef[1, x, :, s] * prev[x, :, s] + coef[2, x, :, s] * total
            ) + inject[step, x, :, s]


def margin(ya, yb, x, s, row):
    _, odd, below, above = place("gy")
    low = kept(below, jnp.where(odd, ya[x, :, s], yb[x, :, s]))
    high = kept(above, jnp.where(odd, yb[x, :, s], ya[x, :, s]))
    return jnp.where(lax.rem(row, 4) == 0, high, low)


def put_margins(get, size_x, count, a_ref, b_ref, at):
    odd = place("gx")[1]
    row = rows()
    outer = (lax.rem(row, 4) == 0) | (lax.rem(row, 4) == 3)
    for i in range((WIDE + 1) // 2):
        for j in range(count):
            sides = []
            for start in (0, size_x - WIDE):
                one = get(start + 2 * i, j)
                if 2 * i + 1 < WIDE:
                    one = jnp.where(outer, one, pltpu.roll(get(start + 2 * i + 1, j), 2, axis=0))
                sides.append(one)
            a_ref[at + i, :, chunk(j)] = jnp.where(odd, sides[0], sides[1])
            b_ref[at + i, :, chunk(j)] = jnp.where(odd, sides[1], sides[0])


def around_x(x, s, cur, xa, xb):
    _, odd, below, above = place("gx")
    size_x = cur.shape[0]
    if x < 0:
        return kept(below, jnp.where(odd, xa[WIDE + x, :, s], xb[WIDE + x, :, s]))
    if x >= size_x:
        return kept(above, jnp.where(odd, xb[x - size_x, :, s], xa[x - size_x, :, s]))
    return cur[x, :, s]


def first_step(cur, prev, coef, inject, xa, xb, ya, yb, new, a_ref, b_ref):
    forward(0, cur, prev, coef, inject, xa, xb, ya, yb, new)
    put_sides(new, a_ref, b_ref, 4)


def second_step(cur, prev, coef, inject, xa, xb, ya, yb, new, a_ref, b_ref):
    forward(1, cur, prev, coef, inject, xa, xb, ya, yb, new)
    put_sides(new, a_ref, b_ref, WIDE)


def third_step(cur, prev, coef, inject, xa, xb, ya, yb, new, a_ref, b_ref):
    forward(2, cur, prev, coef, inject, xa, xb, ya, yb, new)
    size_x, _, size_z = cur.shape
    put_sides(new, a_ref, b_ref, 4)
    row = rows()
    put_margins(lambda x, j: margin(ya, yb, x, chunk(j), row), size_x, size_z // LANES, a_ref, b_ref, 4)


def fourth_step(cur, prev, coef, inject, xa, xb, ya, yb, new, source, receiver, ya_ref, yb_ref):
    forward(3, cur, prev, coef, inject, xa, xb, ya, yb, new)
    size_x, _, size_z = source.shape
    odd = place("gy")[1]
    row = lax.rem(rows(), 4)
    for x in range(size_x):
        source[x] = new[x, 0:4, :size_z]
        receiver[x] = new[x, 4:8, :size_z]
    for i in range(size_x // 4):
        for j in range(size_z // LANES):
            tops, bottoms = [], []
            for q in range(4):
                value = new[4 * i + q, :, chunk(j)]
                tops.append(value if q == 0 else pltpu.roll(value, 8 - q, axis=0))
                bottoms.append(pltpu.roll(value, 3 - q, axis=0) if q < 3 else value)
            high, low = tops[0], bottoms[0]
            for q in range(1, 4):
                high = jnp.where(row == 3 - q, tops[q], high)
                low = jnp.where(row == 3 - q, bottoms[q], low)
            ya_ref[i, :, chunk(j)] = jnp.where(odd, low, high)
            yb_ref[i, :, chunk(j)] = jnp.where(odd, high, low)


def gather_edges(cur, ya, yb, margins, a_ref, b_ref):
    size_x, _, size_z = margins.shape
    _, odd, below, above = place("gy")
    row = lax.rem(rows(), 4)
    for x in range(size_x):
        i, q = divmod(x, 4)
        for j in range(size_z // LANES):
            s = chunk(j)
            low = kept(below, jnp.where(odd, ya[i, :, s], yb[i, :, s]))
            high = kept(above, jnp.where(odd, yb[i, :, s], ya[i, :, s]))
            if q:
                low = pltpu.roll(low, q, axis=0)
            high = pltpu.roll(high, (q + 5) % 8, axis=0)
            margins[x, :, s] = jnp.where(row == 0, high, low)
    put_sides(cur, a_ref, b_ref, WIDE)
    put_margins(lambda x, j: margins[x, :, chunk(j)], size_x, size_z // LANES, a_ref, b_ref, WIDE)


def widen(get_margin, cur, xa, xb, ma, mb, m_at, first_ref, second_ref, first_z, second_z):
    size_x = cur.shape[0]
    size_z = first_ref.shape[2]
    _, odd, below, above = place("gx")
    own = rows() < 4
    for x in range(-WIDE, size_x + WIDE):
        e = x + WIDE
        for j in range(size_z // LANES):
            s = chunk(j)
            if 0 <= x < size_x:
                edge = get_margin(x, s)
            else:
                k = e if x < 0 else x - size_x
                i, other = divmod(k, 2)
                near, far = ma[m_at + i, :, s], mb[m_at + i, :, s]
                edge = kept(below, jnp.where(odd, near, far)) if x < 0 else kept(above, jnp.where(odd, far, near))
                if other:
                    edge = pltpu.roll(edge, 6, axis=0)
            both = around_x(x, s, cur, xa, xb)
            first_ref[e, :, s] = jnp.where(own, both, pltpu.roll(edge, 4, axis=0))
            second_ref[e, :, s] = jnp.where(own, pltpu.roll(both, 4, axis=0), edge)
        beyond = around_x(x, slice(size_z, size_z + LANES), cur, xa, xb)
        first_z[e] = beyond
        second_z[e] = pltpu.roll(beyond, 4, axis=0)


def early(cur, xa, xb, ya, yb, ma, mb, first_ref, second_ref, first_z, second_z):
    row = rows()
    widen(
        lambda x, s: margin(ya, yb, x, s, row), cur, xa, xb, ma, mb, 4,
        first_ref, second_ref, first_z, second_z,
    )


def filtered(s2, r2, s2z, r2z, cur, margins, xa, xb, out, s4, r4, s4z, r4z):
    size_x, _, size_z = margins.shape
    count = size_z // LANES
    widen(lambda x, s: margins[x, :, s], cur, xa, xb, xa, xb, WIDE, s4, r4, s4z, r4z)
    first = lax.axis_index("gz") == 0
    lane = lanes()

    def each(lag, carry):
        def image(x):
            a, b = x - lag + HALF + WIDE, x + lag - HALF + WIDE
            return [
                s2[a, :, chunk(j)] * r2[b, :, chunk(j)] + s4[a, :, chunk(j)] * r4[b, :, chunk(j)]
                for j in range(count)
            ]

        previous, here = image(-1), image(0)
        for x in range(size_x):
            following = image(x + 1)
            a, b = x - lag + HALF + WIDE, x + lag - HALF + WIDE
            beyond = s2z[a] * r2z[b] + s4z[a] * r4z[b]
            before, after = kept(jnp.logical_not(first), beyond), kept(first, beyond)
            up = [pltpu.roll(v, LANES - 1, axis=1) for v in (*here, after)]
            down = [pltpu.roll(v, 1, axis=1) for v in (before, *here)]
            for j in range(count):
                along = jnp.where(lane < LANES - 1, up[j], up[j + 1]) + jnp.where(lane >= 1, down[j + 1], down[j])
                across = pltpu.roll(here[j], 7, axis=0) + pltpu.roll(here[j], 1, axis=0)
                value = 6.0 * here[j] - (previous[j] + following[j] + across + along)
                out[lag, x, :, chunk(j)] = value[0:4].astype(jnp.bfloat16)
            previous, here = here, following
        return carry

    lax.fori_loop(0, LAGS, each, 0)


def local(
    source_prev,
    source_now,
    receiver_prev,
    receiver_now,
    courant,
    absorbing,
    source_cell,
    wavelet,
    receiver_cells,
    traces,
):
    f32 = jnp.float32
    size_x, size_y, size_z = courant.shape
    deep_z = size_z + LANES
    wide_x = size_x + 2 * WIDE
    packed = (WIDE + 1) // 2
    tile = ((size_x, 8, deep_z), f32)
    field = ((size_x, size_y, size_z), f32)

    def side(n, z=size_z):
        return ((n, 8, z), f32)

    outer = side(wide_x), side(wide_x), side(wide_x, LANES), side(wide_x, LANES)
    now, old, medium, z = call(
        merge,
        [side(size_x), side(size_x), side(size_x), side(3 * size_x, LANES)],
        source_now, receiver_now, source_prev, receiver_prev, courant, absorbing,
        far=range(6),
    )
    beyond = cross(z)
    now, a, b = call(pack, [tile, side(4, deep_z), side(4, deep_z)], now, beyond)
    halo0 = (*swap(a, b, "gx"), *swap(now, now, "gy"))
    blocks = receiver_cells.shape[0] // LANES
    coef, prev, inject = call(
        prepare,
        [((3, *tile[0]), f32), tile, ((STEPS, *tile[0]), f32)],
        source_cell, wavelet, receiver_cells.T, traces, old, medium, beyond,
        scratch=[pltpu.VMEM((blocks, 8, LANES), jnp.int32), pltpu.VMEM((STEPS, blocks, 8, LANES), f32)],
        smem=(0, 1),
        far=(2, 3),
    )
    one, a, b = call(first_step, [tile, side(4, deep_z), side(4, deep_z)], now, prev, coef, inject, *halo0)
    halo1 = (*swap(a, b, "gx"), *swap(one, one, "gy"))
    two, a, b = call(second_step, [tile, side(WIDE, deep_z), side(WIDE, deep_z)], one, now, coef, inject, *halo1)
    halo2 = (*swap(a, b, "gx"), *swap(two, two, "gy"))
    three, a, b = call(
        third_step, [tile, side(4 + packed, deep_z), side(4 + packed, deep_z)], two, one, coef, inject, *halo2
    )
    halo3 = (*swap(a, b, "gx"), *swap(three, three, "gy"))
    four, source, receiver, c, d = call(
        fourth_step,
        [tile, field, field, side(size_x // 4), side(size_x // 4)],
        three, two, coef, inject, *halo3,
        far_outs=(1, 2),
    )
    edges = swap(c, d, "gy")
    margins, a, b = call(
        gather_edges,
        [side(size_x), side(WIDE + packed, deep_z), side(WIDE + packed, deep_z)],
        four, *edges,
    )
    halo4 = swap(a, b, "gx")
    before = call(early, outer, two, *halo2, halo3[0], halo3[1])
    (image,) = call(
        filtered,
        [((LAGS, size_x, size_y, size_z), jnp.bfloat16)],
        *before, four, margins, *halo4,
        scratch=[pltpu.VMEM(s, f32) for s, _ in outer],
        far_outs=(0,),
    )
    return source, receiver, image


def solution(mesh):
    placed = (
        P(("shot", "gx"), "gy", "gz"),
        P(("shot", "gx"), "gy", "gz"),
        P(("shot", "gx"), "gy", "gz"),
        P(("shot", "gx"), "gy", "gz"),
        P("gx", "gy", "gz"),
        P("gx", "gy", "gz"),
        P("shot"),
        P("shot"),
        P("shot", None),
        P(None, "shot"),
    )
    return jax.shard_map(
        local,
        mesh=mesh,
        in_specs=placed,
        out_specs=(
            P(("shot", "gx"), "gy", "gz"),
            P(("shot", "gx"), "gy", "gz"),
            P(None, ("shot", "gx"), "gy", "gz"),
        ),
        check_vma=False,
    )
```

```python
import functools

import jax
import jax.numpy as jnp
from jax import lax
from jax.experimental import pallas as pl
from jax.experimental.pallas import tpu as pltpu
from jax.sharding import PartitionSpec as P

LAGS = 16
STEPS = 4
EVERY = 2
LANES = 128
HALF = LAGS // 2
WIDE = HALF + 1

stencil_weights = (8.0 / 5.0, -1.0 / 5.0, 8.0 / 315.0, -1.0 / 560.0)
centre_weight = -205.0 / 72.0


def pairs(size):
    near = [(i, i ^ 1) for i in range(size)]
    far = [(i, (i + 1) % size if i % 2 else (i - 1) % size) for i in range(size)]
    return near, far


def swap(a, b, axis):
    near, far = pairs(lax.axis_size(axis))
    return lax.ppermute(a, axis, near), lax.ppermute(b, axis, far)


def cross(a):
    return lax.all_gather(a, "gz")


def rows():
    return lax.broadcasted_iota(jnp.int32, (8, LANES), 0)


def lanes():
    return lax.broadcasted_iota(jnp.int32, (8, LANES), 1)


def place(axis):
    index = lax.axis_index(axis)
    return index, lax.rem(index, 2) == 1, index > 0, index < lax.axis_size(axis) - 1


def chunk(j):
    return slice(j * LANES, (j + 1) * LANES)


def kept(flag, value):
    return jnp.where(flag, value, jnp.zeros_like(value))


def call(body, outs, *args, scratch=(), smem=(), far=(), far_outs=(), left=()):
    args = [
        a if i in smem else pltpu.with_memory_space_constraint(a, pltpu.HBM if i in far else pltpu.VMEM)
        for i, a in enumerate(args)
    ]
    return pl.pallas_call(
        body,
        out_shape=[
            jax.ShapeDtypeStruct(s, d) if i in far_outs else pltpu.VMEM(s, d)
            for i, (s, d) in enumerate(outs)
        ],
        in_specs=[
            pl.BlockSpec(memory_space=pltpu.SMEM if i in smem else pltpu.VMEM)
            for i in range(len(args))
        ],
        out_specs=[
            pl.BlockSpec(memory_space=pltpu.HBM if i in left else pltpu.VMEM) for i in range(len(outs))
        ],
        scratch_shapes=list(scratch),
        compiler_params=pltpu.CompilerParams(vmem_limit_bytes=8 * 2**20),
        name=body.func.__name__ if isinstance(body, functools.partial) else body.__name__,
    )(*args)


def put_sides(tile, a_ref, b_ref, width):
    odd = place("gx")[1]
    size = tile.shape[0]
    for k in range(width):
        low, high = tile[k], tile[size - width + k]
        a_ref[k] = jnp.where(odd, low, high)
        b_ref[k] = jnp.where(odd, high, low)


def merge(source, receiver, before, behind, courant, absorbing, now, prev, medium, z_ref):
    last = place("gz")[0] == 0
    size_x, _, size_z = source.shape
    for k in range(size_x):
        now[k, 0:4] = source[k]
        now[k, 4:8] = receiver[k]
        prev[k, 0:4] = before[k]
        prev[k, 4:8] = behind[k]
        medium[k, 0:4] = courant[k]
        medium[k, 4:8] = absorbing[k].astype(jnp.float32)
    for n, tile in enumerate((now, prev, medium)):
        for k in range(size_x):
            z_ref[n * size_x + k] = jnp.where(last, tile[k, :, -LANES:], tile[k, :, :LANES])


def pack(now, beyond, tile, a_ref, b_ref):
    size_x, _, size_z = now.shape
    other = 1 - lax.axis_index("gz")
    for k in range(size_x):
        tile[k, :, :size_z] = now[k]
        tile[k, :, size_z:] = beyond[other, k]
    put_sides(tile, a_ref, b_ref, 4)


def prepare(cell, wavelet, spots, traces, old, medium, beyond, coef, prev, inject, code_ref, amp_ref):
    size_x, _, size_z = old.shape
    first = lax.axis_index("gz") == 0
    count = size_z // LANES
    other = 1 - lax.axis_index("gz")
    for k in range(size_x):
        prev[k, :, :size_z] = old[k]
        prev[k, :, size_z:] = beyond[other, size_x + k]
        for j in range(count + 1):
            both = medium[k, :, chunk(j)] if j < count else beyond[other, 2 * size_x + k]
            upper = rows() < 4
            turned = pltpu.roll(both, 4, axis=0)
            courant = jnp.where(upper, both, turned)
            damping = jnp.where(upper, turned, both) / 16.0
            inverse = 1.0 / (1.0 + damping)
            coef[0, k, :, chunk(j)] = 2.0 * inverse
            coef[1, k, :, chunk(j)] = (1.0 - damping) * inverse
            coef[2, k, :, chunk(j)] = courant * inverse
    gx, gy, gz = (lax.axis_index(a) for a in ("gx", "gy", "gz"))
    sx, sy, sz = cell[0] - gx * size_x, cell[1] - gy * 4, cell[2] - gz * size_z
    at_x, at_y = spots[0:1] - gx * size_x, spots[1:2] - gy * 4
    inside = (at_x >= 0) & (at_x < size_x) & (at_y >= 0) & (at_y < 4) & (gz == 0)
    code = jnp.where(inside, at_x * 8 + at_y + 4, -1)
    blocks = code.shape[1] // LANES
    for b in range(blocks):
        code_ref[b] = jnp.broadcast_to(code[:, chunk(b)], (8, LANES))
        for t in range(STEPS):
            amp_ref[t, b] = jnp.broadcast_to(traces[t : t + 1, chunk(b)], (8, LANES))
    row, lane = rows(), lanes()

    def each(k, carry):
        sums = [jnp.zeros((8, LANES), jnp.float32) for _ in range(STEPS)]
        for b in range(blocks):
            hit = code_ref[b] == row + k * 8
            for t in range(STEPS):
                sums[t] = sums[t] + jnp.where(hit, amp_ref[t, b], 0.0)
        for t in range(STEPS):
            sheet = jnp.where(lane == 0, jnp.sum(sums[t], axis=1, keepdims=True), 0.0)
            for j in range(count + 1):
                start = j * LANES if j < count else jnp.where(first, size_z, -LANES)
                spot = (row == sy) & (sy < 4) & (lane + start == sz) & (k == sx)
                point = jnp.where(spot, wavelet[t], 0.0)
                inject[t, k, :, chunk(j)] = point + sheet if j == 0 else point
        return carry

    lax.fori_loop(0, size_x, each, 0)


def forward(step, cur, prev, coef, inject, xa, xb, ya, yb, new):
    size_x, _, size_z = cur.shape
    count = size_z // LANES
    _, odd_x, below_x, above_x = place("gx")
    _, odd_y, below_y, above_y = place("gy")
    first = lax.axis_index("gz") == 0
    second = jnp.logical_not(first)
    wide = xa.shape[0] if step == 2 else 4
    row, lane = lax.rem(rows(), 4), lanes()

    def at(x, j):
        if x < 0:
            return kept(below_x, jnp.where(odd_x, xa[wide + x, :, chunk(j)], xb[wide + x, :, chunk(j)]))
        if x >= size_x:
            return kept(above_x, jnp.where(odd_x, xb[x - size_x, :, chunk(j)], xa[x - size_x, :, chunk(j)]))
        return cur[x, :, chunk(j)]

    for x in range(size_x):
        own = [cur[x, :, chunk(j)] for j in range(count)]
        along = [None] * count
        for k, weight in enumerate(stencil_weights, 1):
            up = [pltpu.roll(v, LANES - k, axis=1) for v in own]
            down = [pltpu.roll(v, k, axis=1) for v in own]
            after = [*up[1 : count - 1], kept(first, up[count - 1]), kept(second, up[0])]
            before = [kept(second, down[count - 1]), *down[: count - 2], kept(first, down[count - 2])]
            for j in range(count):
                both = jnp.where(lane < LANES - k, up[j], after[j]) + jnp.where(lane >= k, down[j], before[j])
                both = both + at(x + k, j) + at(x - k, j)
                along[j] = weight * both if along[j] is None else along[j] + weight * both
        for j in range(count):
            s = chunk(j)
            centre = own[j]
            low = kept(below_y, jnp.where(odd_y, ya[x, :, s], yb[x, :, s]))
            high = kept(above_y, jnp.where(odd_y, yb[x, :, s], ya[x, :, s]))
            total = 3.0 * centre_weight * centre + along[j] + stencil_weights[3] * (low + high)
            for k, weight in enumerate(stencil_weights[:3], 1):
                up = jnp.where(row < 4 - k, pltpu.roll(centre, 8 - k, axis=0), pltpu.roll(high, 4 - k, axis=0))
                down = jnp.where(row >= k, pltpu.roll(centre, k, axis=0), pltpu.roll(low, 4 + k, axis=0))
                total = total + weight * (up + down)
            new[x, :, s] = (
                coef[0, x, :, s] * centre - coef[1, x, :, s] * prev[x, :, s] + coef[2, x, :, s] * total
            ) + inject[step, x, :, s]


def margin(ya, yb, x, s, row):
    _, odd, below, above = place("gy")
    low = kept(below, jnp.where(odd, ya[x, :, s], yb[x, :, s]))
    high = kept(above, jnp.where(odd, yb[x, :, s], ya[x, :, s]))
    return jnp.where(lax.rem(row, 4) == 0, high, low)


def put_margins(get, size_x, count, a_ref, b_ref, at):
    odd = place("gx")[1]
    row = rows()
    outer = (lax.rem(row, 4) == 0) | (lax.rem(row, 4) == 3)
    for i in range((WIDE + 1) // 2):
        for j in range(count):
            sides = []
            for start in (0, size_x - WIDE):
                one = get(start + 2 * i, j)
                if 2 * i + 1 < WIDE:
                    one = jnp.where(outer, one, pltpu.roll(get(start + 2 * i + 1, j), 2, axis=0))
                sides.append(one)
            a_ref[at + i, :, chunk(j)] = jnp.where(odd, sides[0], sides[1])
            b_ref[at + i, :, chunk(j)] = jnp.where(odd, sides[1], sides[0])


def around_x(x, s, cur, xa, xb):
    _, odd, below, above = place("gx")
    size_x = cur.shape[0]
    if x < 0:
        return kept(below, jnp.where(odd, xa[WIDE + x, :, s], xb[WIDE + x, :, s]))
    if x >= size_x:
        return kept(above, jnp.where(odd, xb[x - size_x, :, s], xa[x - size_x, :, s]))
    return cur[x, :, s]


def first_step(cur, prev, coef, inject, xa, xb, ya, yb, new, a_ref, b_ref):
    forward(0, cur, prev, coef, inject, xa, xb, ya, yb, new)
    put_sides(new, a_ref, b_ref, 4)


def second_step(cur, prev, coef, inject, xa, xb, ya, yb, new, a_ref, b_ref):
    forward(1, cur, prev, coef, inject, xa, xb, ya, yb, new)
    put_sides(new, a_ref, b_ref, WIDE)


def third_step(cur, prev, coef, inject, xa, xb, ya, yb, new, a_ref, b_ref):
    forward(2, cur, prev, coef, inject, xa, xb, ya, yb, new)
    size_x, _, size_z = cur.shape
    put_sides(new, a_ref, b_ref, 4)
    row = rows()
    put_margins(lambda x, j: margin(ya, yb, x, chunk(j), row), size_x, size_z // LANES, a_ref, b_ref, 4)


def fourth_step(cur, prev, coef, inject, xa, xb, ya, yb, new, ya_ref, yb_ref):
    forward(3, cur, prev, coef, inject, xa, xb, ya, yb, new)
    size_x = new.shape[0]
    size_z = ya_ref.shape[2]
    odd = place("gy")[1]
    row = lax.rem(rows(), 4)
    for i in range(size_x // 4):
        for j in range(size_z // LANES):
            tops, bottoms = [], []
            for q in range(4):
                value = new[4 * i + q, :, chunk(j)]
                tops.append(value if q == 0 else pltpu.roll(value, 8 - q, axis=0))
                bottoms.append(pltpu.roll(value, 3 - q, axis=0) if q < 3 else value)
            high, low = tops[0], bottoms[0]
            for q in range(1, 4):
                high = jnp.where(row == 3 - q, tops[q], high)
                low = jnp.where(row == 3 - q, bottoms[q], low)
            ya_ref[i, :, chunk(j)] = jnp.where(odd, low, high)
            yb_ref[i, :, chunk(j)] = jnp.where(odd, high, low)


def gather_edges(cur, ya, yb, margins, a_ref, b_ref):
    size_x, _, size_z = margins.shape
    _, odd, below, above = place("gy")
    row = lax.rem(rows(), 4)
    for x in range(size_x):
        i, q = divmod(x, 4)
        for j in range(size_z // LANES):
            s = chunk(j)
            low = kept(below, jnp.where(odd, ya[i, :, s], yb[i, :, s]))
            high = kept(above, jnp.where(odd, yb[i, :, s], ya[i, :, s]))
            if q:
                low = pltpu.roll(low, q, axis=0)
            high = pltpu.roll(high, (q + 5) % 8, axis=0)
            margins[x, :, s] = jnp.where(row == 0, high, low)
    put_sides(cur, a_ref, b_ref, WIDE)
    put_margins(lambda x, j: margins[x, :, chunk(j)], size_x, size_z // LANES, a_ref, b_ref, WIDE)


def widen(get_margin, cur, xa, xb, ma, mb, m_at, first_ref, second_ref, first_z, second_z):
    size_x = cur.shape[0]
    size_z = first_ref.shape[2]
    _, odd, below, above = place("gx")
    own = rows() < 4
    for x in range(-WIDE, size_x + WIDE):
        e = x + WIDE
        for j in range(size_z // LANES):
            s = chunk(j)
            if 0 <= x < size_x:
                edge = get_margin(x, s)
            else:
                k = e if x < 0 else x - size_x
                i, other = divmod(k, 2)
                near, far = ma[m_at + i, :, s], mb[m_at + i, :, s]
                edge = kept(below, jnp.where(odd, near, far)) if x < 0 else kept(above, jnp.where(odd, far, near))
                if other:
                    edge = pltpu.roll(edge, 6, axis=0)
            both = around_x(x, s, cur, xa, xb)
            first_ref[e, :, s] = jnp.where(own, both, pltpu.roll(edge, 4, axis=0))
            second_ref[e, :, s] = jnp.where(own, pltpu.roll(both, 4, axis=0), edge)
        beyond = around_x(x, slice(size_z, size_z + LANES), cur, xa, xb)
        first_z[e] = beyond
        second_z[e] = pltpu.roll(beyond, 4, axis=0)


def laplace(first, second, first_z, second_z, lag, emit):
    size_x = first.shape[0] - 2 * WIDE
    count = first.shape[2] // LANES
    core = lax.axis_index("gz") == 0
    lane = lanes()

    def image(x):
        a, b = x - lag + HALF + WIDE, x + lag - HALF + WIDE
        return [first[a, :, chunk(j)] * second[b, :, chunk(j)] for j in range(count)]

    previous, here = image(-1), image(0)
    for x in range(size_x):
        following = image(x + 1)
        beyond = first_z[x - lag + HALF + WIDE] * second_z[x + lag - HALF + WIDE]
        before, after = kept(jnp.logical_not(core), beyond), kept(core, beyond)
        up = [pltpu.roll(v, LANES - 1, axis=1) for v in (*here, after)]
        down = [pltpu.roll(v, 1, axis=1) for v in (before, *here)]
        for j in range(count):
            along = jnp.where(lane < LANES - 1, up[j], up[j + 1]) + jnp.where(lane >= 1, down[j + 1], down[j])
            across = pltpu.roll(here[j], 7, axis=0) + pltpu.roll(here[j], 1, axis=0)
            emit(x, chunk(j), 6.0 * here[j] - (previous[j] + following[j] + across + along))
        previous, here = here, following


def early(cur, xa, xb, ya, yb, ma, mb, last, partial, source, receiver, *wide):
    row = rows()
    size_x, _, size_z = source.shape
    for x in range(size_x):
        source[x] = last[x, 0:4, :size_z]
        receiver[x] = last[x, 4:8, :size_z]
    widen(lambda x, s: margin(ya, yb, x, s, row), cur, xa, xb, ma, mb, 4, *wide)

    def each(lag, carry):
        def emit(x, s, value):
            partial[lag, x, :, s] = value[0:4]

        laplace(*wide, lag, emit)
        return carry

    lax.fori_loop(0, LAGS, each, 0)


def filtered(partial, cur, margins, xa, xb, out, held, done, *wide):
    widen(lambda x, s: margins[x, :, s], cur, xa, xb, xa, xb, WIDE, *wide)

    def each(lag, carry):
        def emit(x, s, value):
            held[lag, x, :, s] = (partial[lag, x, :, s] + value[0:4]).astype(jnp.bfloat16)

        laplace(*wide, lag, emit)
        pltpu.make_async_copy(held.at[lag], out.at[lag], done.at[lag]).start()
        return carry

    def finish(lag, carry):
        pltpu.make_async_copy(held.at[lag], out.at[lag], done.at[lag]).wait()
        return carry

    lax.fori_loop(0, LAGS, each, 0)
    lax.fori_loop(0, LAGS, finish, 0)


def local(
    source_prev,
    source_now,
    receiver_prev,
    receiver_now,
    courant,
    absorbing,
    source_cell,
    wavelet,
    receiver_cells,
    traces,
):
    f32 = jnp.float32
    size_x, size_y, size_z = courant.shape
    deep_z = size_z + LANES
    wide_x = size_x + 2 * WIDE
    packed = (WIDE + 1) // 2
    tile = ((size_x, 8, deep_z), f32)
    field = ((size_x, size_y, size_z), f32)

    def side(n, z=size_z):
        return ((n, 8, z), f32)

    outer = side(wide_x), side(wide_x), side(wide_x, LANES), side(wide_x, LANES)
    now, old, medium, z = call(
        merge,
        [side(size_x), side(size_x), side(size_x), side(3 * size_x, LANES)],
        source_now, receiver_now, source_prev, receiver_prev, courant, absorbing,
        far=range(6),
    )
    beyond = cross(z)
    now, a, b = call(pack, [tile, side(4, deep_z), side(4, deep_z)], now, beyond)
    halo0 = (*swap(a, b, "gx"), *swap(now, now, "gy"))
    blocks = receiver_cells.shape[0] // LANES
    coef, prev, inject = call(
        prepare,
        [((3, *tile[0]), f32), tile, ((STEPS, *tile[0]), f32)],
        source_cell, wavelet, receiver_cells.T, traces, old, medium, beyond,
        scratch=[pltpu.VMEM((blocks, 8, LANES), jnp.int32), pltpu.VMEM((STEPS, blocks, 8, LANES), f32)],
        smem=(0, 1),
        far=(2, 3),
    )
    one, a, b = call(first_step, [tile, side(4, deep_z), side(4, deep_z)], now, prev, coef, inject, *halo0)
    halo1 = (*swap(a, b, "gx"), *swap(one, one, "gy"))
    two, a, b = call(second_step, [tile, side(WIDE, deep_z), side(WIDE, deep_z)], one, now, coef, inject, *halo1)
    halo2 = (*swap(a, b, "gx"), *swap(two, two, "gy"))
    three, a, b = call(
        third_step, [tile, side(4 + packed, deep_z), side(4 + packed, deep_z)], two, one, coef, inject, *halo2
    )
    halo3 = (*swap(a, b, "gx"), *swap(three, three, "gy"))
    four, c, d = call(
        fourth_step, [tile, side(size_x // 4), side(size_x // 4)], three, two, coef, inject, *halo3
    )
    edges = swap(c, d, "gy")
    margins, a, b = call(
        gather_edges,
        [side(size_x), side(WIDE + packed, deep_z), side(WIDE + packed, deep_z)],
        four, *edges,
    )
    halo4 = swap(a, b, "gx")
    picture = (LAGS, size_x, size_y, size_z)
    wide = [pltpu.VMEM(s, f32) for s, _ in outer]
    partial, source, receiver = call(
        early, [(picture, f32), field, field], two, *halo2, halo3[0], halo3[1], four,
        scratch=wide,
        far_outs=(1, 2),
    )
    (image,) = call(
        filtered,
        [(picture, jnp.bfloat16)],
        partial, four, margins, *halo4,
        scratch=[pltpu.VMEM(picture, jnp.bfloat16), pltpu.SemaphoreType.DMA((LAGS,)), *wide],
        far_outs=(0,),
        left=(0,),
    )
    return source, receiver, image


def solution(mesh):
    placed = (
        P(("shot", "gx"), "gy", "gz"),
        P(("shot", "gx"), "gy", "gz"),
        P(("shot", "gx"), "gy", "gz"),
        P(("shot", "gx"), "gy", "gz"),
        P("gx", "gy", "gz"),
        P("gx", "gy", "gz"),
        P("shot"),
        P("shot"),
        P("shot", None),
        P(None, "shot"),
    )
    return jax.shard_map(
        local,
        mesh=mesh,
        in_specs=placed,
        out_specs=(
            P(("shot", "gx"), "gy", "gz"),
            P(("shot", "gx"), "gy", "gz"),
            P(None, ("shot", "gx"), "gy", "gz"),
        ),
        check_vma=False,
    )
```

```python
import functools

import jax
import jax.numpy as jnp
from jax import lax
from jax.experimental import pallas as pl
from jax.experimental.pallas import tpu as pltpu
from jax.sharding import PartitionSpec as P

LAGS = 16
STEPS = 4
EVERY = 2
LANES = 128
HALF = LAGS // 2
WIDE = HALF + 1

stencil_weights = (8.0 / 5.0, -1.0 / 5.0, 8.0 / 315.0, -1.0 / 560.0)
centre_weight = -205.0 / 72.0


def pairs(size):
    near = [(i, i ^ 1) for i in range(size)]
    far = [(i, (i + 1) % size if i % 2 else (i - 1) % size) for i in range(size)]
    return near, far


def swap(a, b, axis):
    near, far = pairs(lax.axis_size(axis))
    return lax.ppermute(a, axis, near), lax.ppermute(b, axis, far)


def cross(a):
    return lax.all_gather(a, "gz")


def rows():
    return lax.broadcasted_iota(jnp.int32, (8, LANES), 0)


def lanes():
    return lax.broadcasted_iota(jnp.int32, (8, LANES), 1)


def place(axis):
    index = lax.axis_index(axis)
    return index, lax.rem(index, 2) == 1, index > 0, index < lax.axis_size(axis) - 1


def chunk(j):
    return slice(j * LANES, (j + 1) * LANES)


def kept(flag, value):
    return jnp.where(flag, value, jnp.zeros_like(value))


def call(body, outs, *args, scratch=(), smem=(), far=(), far_outs=(), left=()):
    args = [
        pltpu.with_memory_space_constraint(a, pltpu.HBM if i in far else pltpu.VMEM)
        for i, a in enumerate(args)
    ]
    return pl.pallas_call(
        body,
        out_shape=[
            jax.ShapeDtypeStruct(s, d) if i in far_outs else pltpu.VMEM(s, d)
            for i, (s, d) in enumerate(outs)
        ],
        in_specs=[
            pl.BlockSpec(memory_space=pltpu.SMEM if i in smem else pltpu.VMEM)
            for i in range(len(args))
        ],
        out_specs=[
            pl.BlockSpec(memory_space=pltpu.HBM if i in left else pltpu.VMEM) for i in range(len(outs))
        ],
        scratch_shapes=list(scratch),
        compiler_params=pltpu.CompilerParams(vmem_limit_bytes=8 * 2**20),
        name=body.func.__name__ if isinstance(body, functools.partial) else body.__name__,
    )(*args)


def put_sides(tile, a_ref, b_ref, width):
    odd = place("gx")[1]
    size = tile.shape[0]
    for k in range(width):
        low, high = tile[k], tile[size - width + k]
        a_ref[k] = jnp.where(odd, low, high)
        b_ref[k] = jnp.where(odd, high, low)


def merge(source, receiver, before, behind, courant, absorbing, now, prev, medium, z_ref):
    last = place("gz")[0] == 0
    size_x, _, size_z = source.shape
    for k in range(size_x):
        now[k, 0:4] = source[k]
        now[k, 4:8] = receiver[k]
        prev[k, 0:4] = before[k]
        prev[k, 4:8] = behind[k]
        medium[k, 0:4] = courant[k]
        medium[k, 4:8] = absorbing[k].astype(jnp.float32)
    for n, tile in enumerate((now, prev, medium)):
        for k in range(size_x):
            z_ref[n * size_x + k] = jnp.where(last, tile[k, :, -LANES:], tile[k, :, :LANES])


def pack(now, beyond, tile, a_ref, b_ref):
    size_x, _, size_z = now.shape
    other = 1 - lax.axis_index("gz")
    for k in range(size_x):
        tile[k, :, :size_z] = now[k]
        tile[k, :, size_z:] = beyond[other, k]
    put_sides(tile, a_ref, b_ref, 4)


def prepare(cell, wavelet, spots, traces, old, medium, beyond, coef, prev, inject, code_ref, amp_ref):
    size_x, _, size_z = old.shape
    first = lax.axis_index("gz") == 0
    count = size_z // LANES
    other = 1 - lax.axis_index("gz")
    for k in range(size_x):
        prev[k, :, :size_z] = old[k]
        prev[k, :, size_z:] = beyond[other, size_x + k]
        for j in range(count + 1):
            both = medium[k, :, chunk(j)] if j < count else beyond[other, 2 * size_x + k]
            upper = rows() < 4
            turned = pltpu.roll(both, 4, axis=0)
            courant = jnp.where(upper, both, turned)
            damping = jnp.where(upper, turned, both) / 16.0
            inverse = 1.0 / (1.0 + damping)
            coef[0, k, :, chunk(j)] = 2.0 * inverse
            coef[1, k, :, chunk(j)] = (1.0 - damping) * inverse
            coef[2, k, :, chunk(j)] = courant * inverse
    gx, gy, gz = (lax.axis_index(a) for a in ("gx", "gy", "gz"))
    sx, sy, sz = cell[0] - gx * size_x, cell[1] - gy * 4, cell[2] - gz * size_z
    at_x, at_y = spots[0:1] - gx * size_x, spots[1:2] - gy * 4
    inside = (at_x >= 0) & (at_x < size_x) & (at_y >= 0) & (at_y < 4) & (gz == 0)
    code = jnp.where(inside, at_x * 8 + at_y + 4, -1)
    blocks = code.shape[1] // LANES
    for b in range(blocks):
        code_ref[b] = jnp.broadcast_to(code[:, chunk(b)], (8, LANES))
        for t in range(STEPS):
            amp_ref[t, b] = jnp.broadcast_to(traces[t : t + 1, chunk(b)], (8, LANES))
    row, lane = rows(), lanes()

    def each(k, carry):
        sums = [jnp.zeros((8, LANES), jnp.float32) for _ in range(STEPS)]
        for b in range(blocks):
            hit = code_ref[b] == row + k * 8
            for t in range(STEPS):
                sums[t] = sums[t] + jnp.where(hit, amp_ref[t, b], 0.0)
        for t in range(STEPS):
            sheet = jnp.where(lane == 0, jnp.sum(sums[t], axis=1, keepdims=True), 0.0)
            for j in range(count + 1):
                start = j * LANES if j < count else jnp.where(first, size_z, -LANES)
                spot = (row == sy) & (sy < 4) & (lane + start == sz) & (k == sx)
                point = jnp.where(spot, wavelet[t], 0.0)
                inject[t, k, :, chunk(j)] = point + sheet if j == 0 else point
        return carry

    lax.fori_loop(0, size_x, each, 0)


def forward(step, cur, prev, coef, inject, xa, xb, ya, yb, new):
    size_x, _, size_z = cur.shape
    count = size_z // LANES
    _, odd_x, below_x, above_x = place("gx")
    _, odd_y, below_y, above_y = place("gy")
    first = lax.axis_index("gz") == 0
    second = jnp.logical_not(first)
    wide = xa.shape[0] if step == 2 else 4
    row, lane = lax.rem(rows(), 4), lanes()

    def at(x, j):
        if x < 0:
            return kept(below_x, jnp.where(odd_x, xa[wide + x, :, chunk(j)], xb[wide + x, :, chunk(j)]))
        if x >= size_x:
            return kept(above_x, jnp.where(odd_x, xb[x - size_x, :, chunk(j)], xa[x - size_x, :, chunk(j)]))
        return cur[x, :, chunk(j)]

    for x in range(size_x):
        own = [cur[x, :, chunk(j)] for j in range(count)]
        along = [None] * count
        for k, weight in enumerate(stencil_weights, 1):
            up = [pltpu.roll(v, LANES - k, axis=1) for v in own]
            down = [pltpu.roll(v, k, axis=1) for v in own]
            after = [*up[1 : count - 1], kept(first, up[count - 1]), kept(second, up[0])]
            before = [kept(second, down[count - 1]), *down[: count - 2], kept(first, down[count - 2])]
            for j in range(count):
                both = jnp.where(lane < LANES - k, up[j], after[j]) + jnp.where(lane >= k, down[j], before[j])
                both = both + at(x + k, j) + at(x - k, j)
                along[j] = weight * both if along[j] is None else along[j] + weight * both
        for j in range(count):
            s = chunk(j)
            centre = own[j]
            low = kept(below_y, jnp.where(odd_y, ya[x, :, s], yb[x, :, s]))
            high = kept(above_y, jnp.where(odd_y, yb[x, :, s], ya[x, :, s]))
            total = 3.0 * centre_weight * centre + along[j] + stencil_weights[3] * (low + high)
            for k, weight in enumerate(stencil_weights[:3], 1):
                up = jnp.where(row < 4 - k, pltpu.roll(centre, 8 - k, axis=0), pltpu.roll(high, 4 - k, axis=0))
                down = jnp.where(row >= k, pltpu.roll(centre, k, axis=0), pltpu.roll(low, 4 + k, axis=0))
                total = total + weight * (up + down)
            new[x, :, s] = (
                coef[0, x, :, s] * centre - coef[1, x, :, s] * prev[x, :, s] + coef[2, x, :, s] * total
            ) + inject[step, x, :, s]


def margin(ya, yb, x, s, row):
    _, odd, below, above = place("gy")
    low = kept(below, jnp.where(odd, ya[x, :, s], yb[x, :, s]))
    high = kept(above, jnp.where(odd, yb[x, :, s], ya[x, :, s]))
    return jnp.where(lax.rem(row, 4) == 0, high, low)


def put_margins(get, size_x, count, a_ref, b_ref, at):
    odd = place("gx")[1]
    row = rows()
    outer = (lax.rem(row, 4) == 0) | (lax.rem(row, 4) == 3)
    for i in range((WIDE + 1) // 2):
        for j in range(count):
            sides = []
            for start in (0, size_x - WIDE):
                one = get(start + 2 * i, j)
                if 2 * i + 1 < WIDE:
                    one = jnp.where(outer, one, pltpu.roll(get(start + 2 * i + 1, j), 2, axis=0))
                sides.append(one)
            a_ref[at + i, :, chunk(j)] = jnp.where(odd, sides[0], sides[1])
            b_ref[at + i, :, chunk(j)] = jnp.where(odd, sides[1], sides[0])


def around_x(x, s, cur, xa, xb):
    _, odd, below, above = place("gx")
    size_x = cur.shape[0]
    if x < 0:
        return kept(below, jnp.where(odd, xa[WIDE + x, :, s], xb[WIDE + x, :, s]))
    if x >= size_x:
        return kept(above, jnp.where(odd, xb[x - size_x, :, s], xa[x - size_x, :, s]))
    return cur[x, :, s]


def first_step(cur, prev, coef, inject, xa, xb, ya, yb, new, a_ref, b_ref):
    forward(0, cur, prev, coef, inject, xa, xb, ya, yb, new)
    put_sides(new, a_ref, b_ref, 4)


def second_step(cur, prev, coef, inject, xa, xb, ya, yb, new, a_ref, b_ref):
    forward(1, cur, prev, coef, inject, xa, xb, ya, yb, new)
    put_sides(new, a_ref, b_ref, WIDE)


def third_step(cur, prev, coef, inject, xa, xb, ya, yb, new, a_ref, b_ref):
    forward(2, cur, prev, coef, inject, xa, xb, ya, yb, new)
    size_x, _, size_z = cur.shape
    put_sides(new, a_ref, b_ref, 4)
    row = rows()
    put_margins(lambda x, j: margin(ya, yb, x, chunk(j), row), size_x, size_z // LANES, a_ref, b_ref, 4)


def fourth_step(cur, prev, coef, inject, xa, xb, ya, yb, new, ya_ref, yb_ref):
    forward(3, cur, prev, coef, inject, xa, xb, ya, yb, new)
    size_x = new.shape[0]
    size_z = ya_ref.shape[2]
    odd = place("gy")[1]
    row = lax.rem(rows(), 4)
    for i in range(size_x // 4):
        for j in range(size_z // LANES):
            tops, bottoms = [], []
            for q in range(4):
                value = new[4 * i + q, :, chunk(j)]
                tops.append(value if q == 0 else pltpu.roll(value, 8 - q, axis=0))
                bottoms.append(pltpu.roll(value, 3 - q, axis=0) if q < 3 else value)
            high, low = tops[0], bottoms[0]
            for q in range(1, 4):
                high = jnp.where(row == 3 - q, tops[q], high)
                low = jnp.where(row == 3 - q, bottoms[q], low)
            ya_ref[i, :, chunk(j)] = jnp.where(odd, low, high)
            yb_ref[i, :, chunk(j)] = jnp.where(odd, high, low)


def gather_edges(cur, ya, yb, margins, a_ref, b_ref):
    size_x, _, size_z = margins.shape
    _, odd, below, above = place("gy")
    row = lax.rem(rows(), 4)
    for x in range(size_x):
        i, q = divmod(x, 4)
        for j in range(size_z // LANES):
            s = chunk(j)
            low = kept(below, jnp.where(odd, ya[i, :, s], yb[i, :, s]))
            high = kept(above, jnp.where(odd, yb[i, :, s], ya[i, :, s]))
            if q:
                low = pltpu.roll(low, q, axis=0)
            high = pltpu.roll(high, (q + 5) % 8, axis=0)
            margins[x, :, s] = jnp.where(row == 0, high, low)
    put_sides(cur, a_ref, b_ref, WIDE)
    put_margins(lambda x, j: margins[x, :, chunk(j)], size_x, size_z // LANES, a_ref, b_ref, WIDE)


def widen(get_margin, cur, xa, xb, ma, mb, m_at, both_ref, rim_ref, first, second, first_rim, second_rim):
    size_x = cur.shape[0]
    _, odd, below, above = place("gx")
    row = rows()
    for x in range(-WIDE, size_x + WIDE):
        e = x + WIDE
        for j in range(both_ref.shape[2] // LANES):
            both_ref[e, :, chunk(j)] = around_x(x, chunk(j), cur, xa, xb)
        for j in range(rim_ref.shape[2] // LANES):
            s = chunk(j)
            if 0 <= x < size_x:
                edge = get_margin(x, s)
            else:
                k = e if x < 0 else x - size_x
                i, other = divmod(k, 2)
                near, far = ma[m_at + i, :, s], mb[m_at + i, :, s]
                edge = kept(below, jnp.where(odd, near, far)) if x < 0 else kept(above, jnp.where(odd, far, near))
                if other:
                    edge = pltpu.roll(edge, 6, axis=0)
            rim_ref[e, :, s] = jnp.where(
                lax.rem(row, 4) == 3, pltpu.roll(edge, 3, axis=0), pltpu.roll(edge, 5, axis=0)
            )
    own = row < 4
    for source, one, two in ((both_ref, first, second), (rim_ref, first_rim, second_rim)):
        for e in range(size_x + 2 * WIDE):
            for j in range(source.shape[2] // LANES):
                s = chunk(j)
                here = source[e, :, s]
                turned = pltpu.roll(here, 4, axis=0)
                if e >= HALF:
                    one[e, :, s] = jnp.where(own, here, pltpu.roll(source[e - HALF, :, s], 4, axis=0))
                if e + HALF < size_x + 2 * WIDE:
                    two[e, :, s] = jnp.where(own, turned, source[e + HALF, :, s])


def laplace(first, second, first_rim, second_rim, lag, emit):
    size_x = first.shape[0] - 2 * WIDE
    count = first_rim.shape[2] // LANES
    core = lax.axis_index("gz") == 0
    lane, row = lanes(), lax.rem(rows(), 4)

    def product(one, two, x, j):
        return one[x - lag + HALF + WIDE, :, chunk(j)] * two[x + lag - HALF + WIDE, :, chunk(j)]

    def image(x):
        return [product(first, second, x, j) for j in range(count)]

    previous, here = image(-1), image(0)
    for x in range(size_x):
        following = image(x + 1)
        beyond = product(first, second, x, count)
        before, after = kept(jnp.logical_not(core), beyond), kept(core, beyond)
        up = [pltpu.roll(v, LANES - 1, axis=1) for v in (*here, after)]
        down = [pltpu.roll(v, 1, axis=1) for v in (before, *here)]
        for j in range(count):
            rim = product(first_rim, second_rim, x, j)
            along = jnp.where(lane < LANES - 1, up[j], up[j + 1]) + jnp.where(lane >= 1, down[j + 1], down[j])
            across = jnp.where(row == 3, rim, pltpu.roll(here[j], 7, axis=0)) + jnp.where(
                row == 0, rim, pltpu.roll(here[j], 1, axis=0)
            )
            emit(x, chunk(j), 6.0 * here[j] - (previous[j] + following[j] + across + along))
        previous, here = here, following


def early(cur, xa, xb, ya, yb, ma, mb, last, partial, source, receiver, both, rim, *wide):
    row = rows()
    size_x, _, size_z = source.shape
    for x in range(size_x):
        source[x] = last[x, 0:4, :size_z]
        receiver[x] = last[x, 4:8, :size_z]
    widen(lambda x, s: margin(ya, yb, x, s, row), cur, xa, xb, ma, mb, 4, both, rim, *wide)

    def each(lag, carry):
        def emit(x, s, value):
            partial[lag, x, :, s] = value

        laplace(*wide, lag, emit)
        return carry

    lax.fori_loop(0, HALF, each, 0)


def filtered(partial, cur, margins, xa, xb, out, held, done, both, rim, *wide):
    widen(lambda x, s: margins[x, :, s], cur, xa, xb, xa, xb, WIDE, both, rim, *wide)

    def copy(lag):
        return pltpu.make_async_copy(held.at[lag], out.at[lag], done.at[lag])

    def each(lag, carry):
        def emit(x, s, value):
            total = (partial[lag, x, :, s] + value).astype(jnp.bfloat16)
            held[lag, x, :, s] = total[0:4]
            held[lag + HALF, x, :, s] = total[4:8]

        laplace(*wide, lag, emit)
        copy(lag).start()
        copy(lag + HALF).start()
        return carry

    def finish(lag, carry):
        copy(lag).wait()
        return carry

    lax.fori_loop(0, HALF, each, 0)
    lax.fori_loop(0, LAGS, finish, 0)


def local(
    source_prev,
    source_now,
    receiver_prev,
    receiver_now,
    courant,
    absorbing,
    source_cell,
    wavelet,
    receiver_cells,
    traces,
):
    f32 = jnp.float32
    size_x, size_y, size_z = courant.shape
    deep_z = size_z + LANES
    wide_x = size_x + 2 * WIDE
    packed = (WIDE + 1) // 2
    tile = ((size_x, 8, deep_z), f32)
    field = ((size_x, size_y, size_z), f32)

    def side(n, z=size_z):
        return ((n, 8, z), f32)

    deep, flat = side(wide_x, deep_z), side(wide_x)
    now, old, medium, z = call(
        merge,
        [side(size_x), side(size_x), side(size_x), side(3 * size_x, LANES)],
        source_now, receiver_now, source_prev, receiver_prev, courant, absorbing,
        far=range(6),
    )
    beyond = cross(z)
    now, a, b = call(pack, [tile, side(4, deep_z), side(4, deep_z)], now, beyond)
    halo0 = (*swap(a, b, "gx"), *swap(now, now, "gy"))
    blocks = receiver_cells.shape[0] // LANES
    coef, prev, inject = call(
        prepare,
        [((3, *tile[0]), f32), tile, ((STEPS, *tile[0]), f32)],
        source_cell, wavelet, receiver_cells.T, traces, old, medium, beyond,
        scratch=[pltpu.VMEM((blocks, 8, LANES), jnp.int32), pltpu.VMEM((STEPS, blocks, 8, LANES), f32)],
        smem=(0, 1),
        far=range(4),
    )
    one, a, b = call(first_step, [tile, side(4, deep_z), side(4, deep_z)], now, prev, coef, inject, *halo0)
    halo1 = (*swap(a, b, "gx"), *swap(one, one, "gy"))
    two, a, b = call(second_step, [tile, side(WIDE, deep_z), side(WIDE, deep_z)], one, now, coef, inject, *halo1)
    halo2 = (*swap(a, b, "gx"), *swap(two, two, "gy"))
    three, a, b = call(
        third_step, [tile, side(4 + packed, deep_z), side(4 + packed, deep_z)], two, one, coef, inject, *halo2
    )
    halo3 = (*swap(a, b, "gx"), *swap(three, three, "gy"))
    four, c, d = call(
        fourth_step, [tile, side(size_x // 4), side(size_x // 4)], three, two, coef, inject, *halo3
    )
    edges = swap(c, d, "gy")
    margins, a, b = call(
        gather_edges,
        [side(size_x), side(WIDE + packed, deep_z), side(WIDE + packed, deep_z)],
        four, *edges,
    )
    halo4 = swap(a, b, "gx")
    picture = (LAGS, size_x, size_y, size_z)
    wide = [pltpu.VMEM(s, f32) for s, _ in (deep, flat, deep, deep, flat, flat)]
    partial, source, receiver = call(
        early, [((HALF, size_x, 8, size_z), f32), field, field], two, *halo2, halo3[0], halo3[1], four,
        scratch=wide,
        far_outs=(1, 2),
    )
    (image,) = call(
        filtered,
        [(picture, jnp.bfloat16)],
        partial, four, margins, *halo4,
        scratch=[pltpu.VMEM(picture, jnp.bfloat16), pltpu.SemaphoreType.DMA((LAGS,)), *wide],
        far_outs=(0,),
        left=(0,),
    )
    return source, receiver, image


def solution(mesh):
    placed = (
        P(("shot", "gx"), "gy", "gz"),
        P(("shot", "gx"), "gy", "gz"),
        P(("shot", "gx"), "gy", "gz"),
        P(("shot", "gx"), "gy", "gz"),
        P("gx", "gy", "gz"),
        P("gx", "gy", "gz"),
        P("shot"),
        P("shot"),
        P("shot", None),
        P(None, "shot"),
    )
    return jax.shard_map(
        local,
        mesh=mesh,
        in_specs=placed,
        out_specs=(
            P(("shot", "gx"), "gy", "gz"),
            P(("shot", "gx"), "gy", "gz"),
            P(None, ("shot", "gx"), "gy", "gz"),
        ),
        check_vma=False,
    )
```

```python
import functools

import jax
import jax.numpy as jnp
from jax import lax
from jax.experimental import pallas as pl
from jax.experimental.pallas import tpu as pltpu
from jax.sharding import PartitionSpec as P

LAGS = 16
STEPS = 4
EVERY = 2
LANES = 128
HALF = LAGS // 2
WIDE = HALF + 1

stencil_weights = (8.0 / 5.0, -1.0 / 5.0, 8.0 / 315.0, -1.0 / 560.0)
centre_weight = -205.0 / 72.0


def pairs(size):
    near = [(i, i ^ 1) for i in range(size)]
    far = [(i, i + 1 if i % 2 else i - 1) for i in range(1, size - 1)]
    return near, far


def swap(a, b, axis):
    near, far = pairs(lax.axis_size(axis))
    return lax.ppermute(a, axis, near), lax.ppermute(b, axis, far)


def cross(a):
    return lax.all_gather(a, "gz")


def rows():
    return lax.broadcasted_iota(jnp.int32, (8, LANES), 0)


def lanes():
    return lax.broadcasted_iota(jnp.int32, (8, LANES), 1)


def place(axis):
    index = lax.axis_index(axis)
    return index, lax.rem(index, 2) == 1, index > 0, index < lax.axis_size(axis) - 1


def chunk(j):
    return slice(j * LANES, (j + 1) * LANES)


def kept(flag, value):
    return jnp.where(flag, value, jnp.zeros_like(value))


def call(body, outs, *args, scratch=(), smem=(), far=(), far_outs=(), left=()):
    args = [
        pltpu.with_memory_space_constraint(a, pltpu.HBM if i in far else pltpu.VMEM)
        for i, a in enumerate(args)
    ]
    return pl.pallas_call(
        body,
        out_shape=[
            jax.ShapeDtypeStruct(s, d) if i in far_outs else pltpu.VMEM(s, d)
            for i, (s, d) in enumerate(outs)
        ],
        in_specs=[
            pl.BlockSpec(memory_space=pltpu.SMEM if i in smem else pltpu.VMEM)
            for i in range(len(args))
        ],
        out_specs=[
            pl.BlockSpec(memory_space=pltpu.HBM if i in left else pltpu.VMEM) for i in range(len(outs))
        ],
        scratch_shapes=list(scratch),
        compiler_params=pltpu.CompilerParams(vmem_limit_bytes=8 * 2**20),
        name=body.func.__name__ if isinstance(body, functools.partial) else body.__name__,
    )(*args)


def put_sides(tile, a_ref, b_ref, width):
    odd = place("gx")[1]
    size = tile.shape[0]
    for k in range(width):
        low, high = tile[k], tile[size - width + k]
        a_ref[k] = jnp.where(odd, low, high)
        b_ref[k] = jnp.where(odd, high, low)


def merge(source, receiver, before, behind, courant, absorbing, now, prev, medium, z_ref):
    last = place("gz")[0] == 0
    size_x, _, size_z = source.shape
    for k in range(size_x):
        now[k, 0:4] = source[k]
        now[k, 4:8] = receiver[k]
        prev[k, 0:4] = before[k]
        prev[k, 4:8] = behind[k]
        medium[k, 0:4] = courant[k]
        medium[k, 4:8] = absorbing[k].astype(jnp.float32)
    for n, tile in enumerate((now, prev, medium)):
        for k in range(size_x):
            z_ref[n * size_x + k] = jnp.where(last, tile[k, :, -LANES:], tile[k, :, :LANES])


def pack(now, beyond, tile, a_ref, b_ref):
    size_x, _, size_z = now.shape
    other = 1 - lax.axis_index("gz")
    for k in range(size_x):
        tile[k, :, :size_z] = now[k]
        tile[k, :, size_z:] = beyond[other, k]
    put_sides(tile, a_ref, b_ref, 4)


def prepare(cell, wavelet, spots, traces, old, medium, beyond, coef, prev, inject, code_ref, amp_ref):
    size_x, _, size_z = old.shape
    first = lax.axis_index("gz") == 0
    count = size_z // LANES
    other = 1 - lax.axis_index("gz")
    for k in range(size_x):
        prev[k, :, :size_z] = old[k]
        prev[k, :, size_z:] = beyond[other, size_x + k]
        for j in range(count + 1):
            both = medium[k, :, chunk(j)] if j < count else beyond[other, 2 * size_x + k]
            upper = rows() < 4
            turned = pltpu.roll(both, 4, axis=0)
            courant = jnp.where(upper, both, turned)
            damping = jnp.where(upper, turned, both) / 16.0
            inverse = 1.0 / (1.0 + damping)
            coef[0, k, :, chunk(j)] = 2.0 * inverse
            coef[1, k, :, chunk(j)] = (1.0 - damping) * inverse
            coef[2, k, :, chunk(j)] = courant * inverse
    gx, gy, gz = (lax.axis_index(a) for a in ("gx", "gy", "gz"))
    sx, sy, sz = cell[0] - gx * size_x, cell[1] - gy * 4, cell[2] - gz * size_z
    at_x, at_y = spots[0:1] - gx * size_x, spots[1:2] - gy * 4
    inside = (at_x >= 0) & (at_x < size_x) & (at_y >= 0) & (at_y < 4) & (gz == 0)
    code = jnp.where(inside, at_x * 8 + at_y + 4, -1)
    blocks = code.shape[1] // LANES
    for b in range(blocks):
        code_ref[b] = jnp.broadcast_to(code[:, chunk(b)], (8, LANES))
        for t in range(STEPS):
            amp_ref[t, b] = jnp.broadcast_to(traces[t : t + 1, chunk(b)], (8, LANES))
    row, lane = rows(), lanes()

    def each(k, carry):
        sums = [jnp.zeros((8, LANES), jnp.float32) for _ in range(STEPS)]
        for b in range(blocks):
            hit = code_ref[b] == row + k * 8
            for t in range(STEPS):
                sums[t] = sums[t] + jnp.where(hit, amp_ref[t, b], 0.0)
        for t in range(STEPS):
            sheet = jnp.where(lane == 0, jnp.sum(sums[t], axis=1, keepdims=True), 0.0)
            for j in range(count + 1):
                start = j * LANES if j < count else jnp.where(first, size_z, -LANES)
                spot = (row == sy) & (sy < 4) & (lane + start == sz) & (k == sx)
                point = jnp.where(spot, wavelet[t], 0.0)
                inject[t, k, :, chunk(j)] = point + sheet if j == 0 else point
        return carry

    lax.fori_loop(0, size_x, each, 0)


def forward(step, cur, prev, coef, inject, xa, xb, ya, yb, new):
    size_x, _, size_z = cur.shape
    count = size_z // LANES
    _, odd_x, below_x, above_x = place("gx")
    _, odd_y, below_y, above_y = place("gy")
    first = lax.axis_index("gz") == 0
    second = jnp.logical_not(first)
    wide = xa.shape[0] if step == 2 else 4
    row, lane = lax.rem(rows(), 4), lanes()

    def at(x, j):
        if x < 0:
            return kept(below_x, jnp.where(odd_x, xa[wide + x, :, chunk(j)], xb[wide + x, :, chunk(j)]))
        if x >= size_x:
            return kept(above_x, jnp.where(odd_x, xb[x - size_x, :, chunk(j)], xa[x - size_x, :, chunk(j)]))
        return cur[x, :, chunk(j)]

    for x in range(size_x):
        own = [cur[x, :, chunk(j)] for j in range(count)]
        along = [None] * count
        for k, weight in enumerate(stencil_weights, 1):
            up = [pltpu.roll(v, LANES - k, axis=1) for v in own]
            down = [pltpu.roll(v, k, axis=1) for v in own]
            after = [*up[1 : count - 1], kept(first, up[count - 1]), kept(second, up[0])]
            before = [kept(second, down[count - 1]), *down[: count - 2], kept(first, down[count - 2])]
            for j in range(count):
                both = jnp.where(lane < LANES - k, up[j], after[j]) + jnp.where(lane >= k, down[j], before[j])
                both = both + at(x + k, j) + at(x - k, j)
                along[j] = weight * both if along[j] is None else along[j] + weight * both
        for j in range(count):
            s = chunk(j)
            centre = own[j]
            low = kept(below_y, jnp.where(odd_y, ya[x, :, s], yb[x, :, s]))
            high = kept(above_y, jnp.where(odd_y, yb[x, :, s], ya[x, :, s]))
            total = 3.0 * centre_weight * centre + along[j] + stencil_weights[3] * (low + high)
            for k, weight in enumerate(stencil_weights[:3], 1):
                up = jnp.where(row < 4 - k, pltpu.roll(centre, 8 - k, axis=0), pltpu.roll(high, 4 - k, axis=0))
                down = jnp.where(row >= k, pltpu.roll(centre, k, axis=0), pltpu.roll(low, 4 + k, axis=0))
                total = total + weight * (up + down)
            new[x, :, s] = (
                coef[0, x, :, s] * centre - coef[1, x, :, s] * prev[x, :, s] + coef[2, x, :, s] * total
            ) + inject[step, x, :, s]


def margin(ya, yb, x, s, row):
    _, odd, below, above = place("gy")
    low = kept(below, jnp.where(odd, ya[x, :, s], yb[x, :, s]))
    high = kept(above, jnp.where(odd, yb[x, :, s], ya[x, :, s]))
    return jnp.where(lax.rem(row, 4) == 0, high, low)


def put_margins(get, size_x, count, a_ref, b_ref, at):
    odd = place("gx")[1]
    row = rows()
    outer = (lax.rem(row, 4) == 0) | (lax.rem(row, 4) == 3)
    for i in range((WIDE + 1) // 2):
        for j in range(count):
            sides = []
            for start in (0, size_x - WIDE):
                one = get(start + 2 * i, j)
                if 2 * i + 1 < WIDE:
                    one = jnp.where(outer, one, pltpu.roll(get(start + 2 * i + 1, j), 2, axis=0))
                sides.append(one)
            a_ref[at + i, :, chunk(j)] = jnp.where(odd, sides[0], sides[1])
            b_ref[at + i, :, chunk(j)] = jnp.where(odd, sides[1], sides[0])


def around_x(x, s, cur, xa, xb):
    _, odd, below, above = place("gx")
    size_x = cur.shape[0]
    if x < 0:
        return kept(below, jnp.where(odd, xa[WIDE + x, :, s], xb[WIDE + x, :, s]))
    if x >= size_x:
        return kept(above, jnp.where(odd, xb[x - size_x, :, s], xa[x - size_x, :, s]))
    return cur[x, :, s]


def first_step(cur, prev, coef, inject, xa, xb, ya, yb, new, a_ref, b_ref):
    forward(0, cur, prev, coef, inject, xa, xb, ya, yb, new)
    put_sides(new, a_ref, b_ref, 4)


def second_step(cur, prev, coef, inject, xa, xb, ya, yb, new, a_ref, b_ref):
    forward(1, cur, prev, coef, inject, xa, xb, ya, yb, new)
    put_sides(new, a_ref, b_ref, WIDE)


def third_step(cur, prev, coef, inject, xa, xb, ya, yb, new, a_ref, b_ref):
    forward(2, cur, prev, coef, inject, xa, xb, ya, yb, new)
    size_x, _, size_z = cur.shape
    put_sides(new, a_ref, b_ref, 4)
    row = rows()
    put_margins(lambda x, j: margin(ya, yb, x, chunk(j), row), size_x, size_z // LANES, a_ref, b_ref, 4)


def fourth_step(cur, prev, coef, inject, xa, xb, ya, yb, new, ya_ref, yb_ref):
    forward(3, cur, prev, coef, inject, xa, xb, ya, yb, new)
    size_x = new.shape[0]
    size_z = ya_ref.shape[2]
    odd = place("gy")[1]
    row = lax.rem(rows(), 4)
    for i in range(size_x // 4):
        for j in range(size_z // LANES):
            tops, bottoms = [], []
            for q in range(4):
                value = new[4 * i + q, :, chunk(j)]
                tops.append(value if q == 0 else pltpu.roll(value, 8 - q, axis=0))
                bottoms.append(pltpu.roll(value, 3 - q, axis=0) if q < 3 else value)
            high, low = tops[0], bottoms[0]
            for q in range(1, 4):
                high = jnp.where(row == 3 - q, tops[q], high)
                low = jnp.where(row == 3 - q, bottoms[q], low)
            ya_ref[i, :, chunk(j)] = jnp.where(odd, low, high)
            yb_ref[i, :, chunk(j)] = jnp.where(odd, high, low)


def gather_edges(cur, ya, yb, margins, a_ref, b_ref):
    size_x, _, size_z = margins.shape
    _, odd, below, above = place("gy")
    row = lax.rem(rows(), 4)
    for x in range(size_x):
        i, q = divmod(x, 4)
        for j in range(size_z // LANES):
            s = chunk(j)
            low = kept(below, jnp.where(odd, ya[i, :, s], yb[i, :, s]))
            high = kept(above, jnp.where(odd, yb[i, :, s], ya[i, :, s]))
            if q:
                low = pltpu.roll(low, q, axis=0)
            high = pltpu.roll(high, (q + 5) % 8, axis=0)
            margins[x, :, s] = jnp.where(row == 0, high, low)
    put_sides(cur, a_ref, b_ref, WIDE)
    put_margins(lambda x, j: margins[x, :, chunk(j)], size_x, size_z // LANES, a_ref, b_ref, WIDE)


def widen(get_margin, cur, xa, xb, ma, mb, m_at, both_ref, rim_ref, first, second, first_rim, second_rim):
    size_x = cur.shape[0]
    _, odd, below, above = place("gx")
    row = rows()
    for x in range(-WIDE, size_x + WIDE):
        e = x + WIDE
        for j in range(both_ref.shape[2] // LANES):
            both_ref[e, :, chunk(j)] = around_x(x, chunk(j), cur, xa, xb)
        for j in range(rim_ref.shape[2] // LANES):
            s = chunk(j)
            if 0 <= x < size_x:
                edge = get_margin(x, s)
            else:
                k = e if x < 0 else x - size_x
                i, other = divmod(k, 2)
                near, far = ma[m_at + i, :, s], mb[m_at + i, :, s]
                edge = kept(below, jnp.where(odd, near, far)) if x < 0 else kept(above, jnp.where(odd, far, near))
                if other:
                    edge = pltpu.roll(edge, 6, axis=0)
            rim_ref[e, :, s] = jnp.where(
                lax.rem(row, 4) == 3, pltpu.roll(edge, 3, axis=0), pltpu.roll(edge, 5, axis=0)
            )
    own = row < 4
    for source, one, two in ((both_ref, first, second), (rim_ref, first_rim, second_rim)):
        for e in range(size_x + 2 * WIDE):
            for j in range(source.shape[2] // LANES):
                s = chunk(j)
                here = source[e, :, s]
                turned = pltpu.roll(here, 4, axis=0)
                if e >= HALF:
                    one[e, :, s] = jnp.where(own, here, pltpu.roll(source[e - HALF, :, s], 4, axis=0))
                if e + HALF < size_x + 2 * WIDE:
                    two[e, :, s] = jnp.where(own, turned, source[e + HALF, :, s])


def laplace(first, second, first_rim, second_rim, lag, emit):
    size_x = first.shape[0] - 2 * WIDE
    count = first_rim.shape[2] // LANES
    core = lax.axis_index("gz") == 0
    lane, row = lanes(), lax.rem(rows(), 4)

    def product(one, two, x, j):
        return one[x - lag + HALF + WIDE, :, chunk(j)] * two[x + lag - HALF + WIDE, :, chunk(j)]

    def image(x):
        return [product(first, second, x, j) for j in range(count)]

    previous, here = image(-1), image(0)
    for x in range(size_x):
        following = image(x + 1)
        beyond = product(first, second, x, count)
        before, after = kept(jnp.logical_not(core), beyond), kept(core, beyond)
        up = [pltpu.roll(v, LANES - 1, axis=1) for v in (*here, after)]
        down = [pltpu.roll(v, 1, axis=1) for v in (before, *here)]
        for j in range(count):
            rim = product(first_rim, second_rim, x, j)
            along = jnp.where(lane < LANES - 1, up[j], up[j + 1]) + jnp.where(lane >= 1, down[j + 1], down[j])
            across = jnp.where(row == 3, rim, pltpu.roll(here[j], 7, axis=0)) + jnp.where(
                row == 0, rim, pltpu.roll(here[j], 1, axis=0)
            )
            emit(x, chunk(j), 6.0 * here[j] - (previous[j] + following[j] + across + along))
        previous, here = here, following


def early(cur, xa, xb, ya, yb, ma, mb, last, partial, source, receiver, both, rim, *wide):
    row = rows()
    size_x, _, size_z = source.shape
    for x in range(size_x):
        source[x] = last[x, 0:4, :size_z]
        receiver[x] = last[x, 4:8, :size_z]
    widen(lambda x, s: margin(ya, yb, x, s, row), cur, xa, xb, ma, mb, 4, both, rim, *wide)

    def each(lag, carry):
        def emit(x, s, value):
            partial[lag, x, :, s] = value

        laplace(*wide, lag, emit)
        return carry

    lax.fori_loop(0, HALF, each, 0)


def filtered(partial, cur, margins, xa, xb, out, held, done, both, rim, *wide):
    widen(lambda x, s: margins[x, :, s], cur, xa, xb, xa, xb, WIDE, both, rim, *wide)

    def copy(lag):
        return pltpu.make_async_copy(held.at[lag], out.at[lag], done.at[lag])

    def each(lag, carry):
        def emit(x, s, value):
            total = (partial[lag, x, :, s] + value).astype(jnp.bfloat16)
            held[lag, x, :, s] = total[0:4]
            held[lag + HALF, x, :, s] = total[4:8]

        laplace(*wide, lag, emit)
        copy(lag).start()
        copy(lag + HALF).start()
        return carry

    def finish(lag, carry):
        copy(lag).wait()
        return carry

    lax.fori_loop(0, HALF, each, 0)
    lax.fori_loop(0, LAGS, finish, 0)


def local(
    source_prev,
    source_now,
    receiver_prev,
    receiver_now,
    courant,
    absorbing,
    source_cell,
    wavelet,
    receiver_cells,
    traces,
):
    f32 = jnp.float32
    size_x, size_y, size_z = courant.shape
    deep_z = size_z + LANES
    wide_x = size_x + 2 * WIDE
    packed = (WIDE + 1) // 2
    tile = ((size_x, 8, deep_z), f32)
    field = ((size_x, size_y, size_z), f32)

    def side(n, z=size_z):
        return ((n, 8, z), f32)

    deep, flat = side(wide_x, deep_z), side(wide_x)
    now, old, medium, z = call(
        merge,
        [side(size_x), side(size_x), side(size_x), side(3 * size_x, LANES)],
        source_now, receiver_now, source_prev, receiver_prev, courant, absorbing,
        far=range(6),
    )
    beyond = cross(z)
    now, a, b = call(pack, [tile, side(4, deep_z), side(4, deep_z)], now, beyond)
    halo0 = (*swap(a, b, "gx"), *swap(now, now, "gy"))
    blocks = receiver_cells.shape[0] // LANES
    coef, prev, inject = call(
        prepare,
        [((3, *tile[0]), f32), tile, ((STEPS, *tile[0]), f32)],
        source_cell, wavelet, receiver_cells.T, traces, old, medium, beyond,
        scratch=[pltpu.VMEM((blocks, 8, LANES), jnp.int32), pltpu.VMEM((STEPS, blocks, 8, LANES), f32)],
        smem=(0, 1),
        far=range(4),
    )
    one, a, b = call(first_step, [tile, side(4, deep_z), side(4, deep_z)], now, prev, coef, inject, *halo0)
    halo1 = (*swap(a, b, "gx"), *swap(one, one, "gy"))
    two, a, b = call(second_step, [tile, side(WIDE, deep_z), side(WIDE, deep_z)], one, now, coef, inject, *halo1)
    halo2 = (*swap(a, b, "gx"), *swap(two, two, "gy"))
    three, a, b = call(
        third_step, [tile, side(4 + packed, deep_z), side(4 + packed, deep_z)], two, one, coef, inject, *halo2
    )
    halo3 = (*swap(a, b, "gx"), *swap(three, three, "gy"))
    four, c, d = call(
        fourth_step, [tile, side(size_x // 4), side(size_x // 4)], three, two, coef, inject, *halo3
    )
    edges = swap(c, d, "gy")
    margins, a, b = call(
        gather_edges,
        [side(size_x), side(WIDE + packed, deep_z), side(WIDE + packed, deep_z)],
        four, *edges,
    )
    halo4 = swap(a, b, "gx")
    picture = (LAGS, size_x, size_y, size_z)
    wide = [pltpu.VMEM(s, f32) for s, _ in (deep, flat, deep, deep, flat, flat)]
    partial, source, receiver = call(
        early, [((HALF, size_x, 8, size_z), f32), field, field], two, *halo2, halo3[0], halo3[1], four,
        scratch=wide,
        far_outs=(1, 2),
    )
    (image,) = call(
        filtered,
        [(picture, jnp.bfloat16)],
        partial, four, margins, *halo4,
        scratch=[pltpu.VMEM(picture, jnp.bfloat16), pltpu.SemaphoreType.DMA((LAGS,)), *wide],
        far_outs=(0,),
        left=(0,),
    )
    return source, receiver, image


def solution(mesh):
    placed = (
        P(("shot", "gx"), "gy", "gz"),
        P(("shot", "gx"), "gy", "gz"),
        P(("shot", "gx"), "gy", "gz"),
        P(("shot", "gx"), "gy", "gz"),
        P("gx", "gy", "gz"),
        P("gx", "gy", "gz"),
        P("shot"),
        P("shot"),
        P("shot", None),
        P(None, "shot"),
    )
    return jax.shard_map(
        local,
        mesh=mesh,
        in_specs=placed,
        out_specs=(
            P(("shot", "gx"), "gy", "gz"),
            P(("shot", "gx"), "gy", "gz"),
            P(None, ("shot", "gx"), "gy", "gz"),
        ),
        check_vma=False,
    )
```
